32 devices in a mesh: seq: 4 (over z), head: 8 (over y, x, core).
Axes of the slice: x: 2, y: 2, z: 4, core: 2. Of those that a mesh axis runs over, the one named last changes fastest.
Arguments:
- query: bfloat16 [8192, 1024], P('seq', 'head'), may hold values from -15 to 15
- key: bfloat16 [8192, 1024], P('seq', 'head'), may hold values from -6 to 6
- value: bfloat16 [8192, 1024], P('seq', 'head'), may hold values from -50 to 50
- grad_out: bfloat16 [8192, 1024], P('seq', 'head'), may hold values from -6 to 6
- log_decay: float32 [8, 8192], P('head', 'seq'), may hold values from -2.5 to 0
- gain: float32 [1024], P('head'), may hold values from 0.25 to 1.75
Outputs:
- grad_query: bfloat16 [8192, 1024], P('seq', 'head')
- grad_key: bfloat16 [8192, 1024], P('seq', 'head')
- grad_value: bfloat16 [8192, 1024], P('seq', 'head')
The draws below stay inside these ranges and needn't reach their ends.
All inputs are finite; a program needn't handle non-finite values.
Results may differ from the reference program's by a relative error of at most 0.0063.
Values sent between devices are 32-bit elements; how exact they have to be, the bound alone decides.
A program may use at most 64 MiB of HBM per device.

```python
import math
import jax
import jax.numpy as jnp
from jax import lax

DH = 128
BLK = 512
TOK_DEV = 2048
HEADS = 8
TOKENS = 8192


def draw_query(key, part):
    first, second = jax.random.split(jax.random.fold_in(key, 11))
    rows = jnp.exp(jax.random.uniform(second, (TOKENS, 1), minval=math.log(0.3), maxval=math.log(3.0)))
    base = jnp.clip(jax.random.normal(first, (TOKENS, HEADS * DH)), -5.0, 5.0)
    return (base * rows).astype(jnp.bfloat16)


def draw_value(key, part):
    first, second = jax.random.split(jax.random.fold_in(key, 17))
    rising = 3.0 ** (jnp.arange(HEADS, dtype=jnp.float32) / max(HEADS - 1, 1))
    spread = jnp.exp(jax.random.uniform(second, (HEADS,), minval=0.0, maxval=math.log(3.3)))
    scales = jnp.repeat(rising * spread, DH)[None, :]
    base = jnp.clip(jax.random.normal(first, (TOKENS, HEADS * DH)), -5.0, 5.0)
    return (base * scales).astype(jnp.bfloat16)


def draw_log_decay(key, part):
    keys = jax.random.split(jax.random.fold_in(key, 29), 7)
    share = 0.5
    quick = jax.random.uniform(keys[0], (HEADS, 1)) < share
    quick_rate = jnp.exp(jax.random.uniform(keys[1], (HEADS, 1), minval=math.log(1.0 / 50.0), maxval=math.log(1.0 / 25.0)))
    keep = jax.random.uniform(keys[2], (HEADS, 1), minval=0.5, maxval=0.7)
    slow_rate = -jnp.log(keep) / TOKENS
    forgetting_factor = jnp.where(quick, quick_rate, slow_rate)
    segments = TOKENS // TOK_DEV
    piece_number = jnp.exp(jax.random.uniform(keys[3], (HEADS, segments, 1), minval=math.log(0.6), maxval=math.log(1.6)))
    piece_number = jnp.broadcast_to(piece_number, (HEADS, segments, TOK_DEV)).reshape(HEADS, TOKENS)
    element_lines = jax.random.uniform(keys[4], (HEADS, TOKENS), minval=0.5, maxval=1.5)
    spots = jax.random.randint(keys[5], (3,), 0, TOKENS)
    scalar_multiplier = jnp.log(jax.random.uniform(keys[6], (HEADS, 3), minval=0.5, maxval=0.8))
    matched_destinations = jnp.arange(TOKENS)[None, :, None] == spots[None, None, :]
    spike_occurrences = jnp.sum(jnp.where(matched_destinations, scalar_multiplier[:, None, :], 0.0), axis=-1)
    return (-forgetting_factor * piece_number * element_lines + spike_occurrences).astype(jnp.float32)


def block_levels(rng, shape, cuts, low, top_value):
    loudness, own = 1.0, jax.random.fold_in(rng, 6)
    for axis_at, parts in cuts:
        steps = jnp.exp(jax.random.uniform(jax.random.fold_in(own, axis_at), (parts,), jnp.float32, low / len(cuts), top_value / len(cuts)))
        loudness = loudness * jnp.repeat(steps, shape[axis_at] // parts).reshape([-1 if axis == axis_at else 1 for axis in range(len(shape))])
    return loudness


def bell_draw(rng, dims, scale, most, cuts=(), kind=jnp.bfloat16):
    values = scale * jax.random.normal(rng, dims, jnp.float32)
    if cuts:
        values = values * block_levels(rng, dims, cuts, -0.22, 0.18)
    return jnp.clip(values, -most, most).astype(kind)


def setup_inputs(seed: int = 0) -> dict:
    splits = jax.random.split(jax.random.key(seed), 7)
    query = draw_query(jax.random.fold_in(splits[6], 71), 0)
    key = bell_draw(splits[1], (TOKENS, HEADS * DH), 1.0, 6.0, ((0, 4), (1, 8)))
    value = draw_value(jax.random.fold_in(splits[6], 71), 0)
    grad_out = bell_draw(splits[3], (TOKENS, HEADS * DH), 1.0, 6.0, ((0, 4), (1, 8)))
    log_decay = draw_log_decay(jax.random.fold_in(splits[6], 71), 0)
    gain = jnp.clip(1.0 + 0.15 * jax.random.normal(splits[5], (HEADS * DH,), jnp.float32), 0.25, 1.75)
    return {"query": query, "key": key, "value": value, "grad_out": grad_out, "log_decay": log_decay, "gain": gain}


EPS = 1e-06

def rounded(x):
    return lax.optimization_barrier(x.astype(jnp.bfloat16)).astype(jnp.float32)

def reference(query, key, value, grad_out, log_decay, gain):
    f32 = jnp.float32
    nblk = TOKENS // BLK
    features = HEADS * DH

    def blocks(x):
        return x.reshape(nblk, BLK, HEADS, DH).transpose(0, 2, 1, 3)
    qb, kb, vb, yb = (blocks(query), blocks(key), blocks(value), blocks(grad_out))
    gains = gain.reshape(HEADS, 1, DH).astype(f32)
    decays = log_decay.reshape(HEADS, nblk, BLK).transpose(1, 0, 2)
    places = jnp.arange(BLK)
    lower = places[:, None] >= places[None, :]

    def tables(block_decay):
        running = jnp.cumsum(block_decay, axis=-1)
        inner = jnp.exp(jnp.where(lower, running[:, :, None] - running[:, None, :], -jnp.inf))
        return (running, running[:, -1], inner)

    def forward(state, inputs):
        qry, kys, vls, grads, block_decay = inputs
        running, last, inner = tables(block_decay)
        qf, kf, vf = (qry.astype(f32), kys.astype(f32), vls.astype(f32))
        mixing = rounded(inner * jnp.einsum('htd,hsd->hts', qf, kf))
        held = rounded(state)
        start = jnp.exp(running)[:, :, None]
        out = jnp.einsum('hts,hsd->htd', mixing, vf) + start * jnp.einsum('htd,hde->hte', qf, held)
        scaled = gains * grads.astype(f32)
        energy = lax.optimization_barrier(jnp.sum(out * out, axis=(0, 2)))
        cross = lax.optimization_barrier(jnp.sum(out * scaled, axis=(0, 2)))
        inv = lax.rsqrt(energy / features + EPS)[None, :, None]
        dout = rounded(inv * scaled - out * (inv ** 3 * cross[None, :, None] / features))
        dmix = rounded(inner * jnp.einsum('hte,hse->hts', dout, vf))
        grad_q = jnp.einsum('hts,hsd->htd', dmix, kf) + start * jnp.einsum('hte,hde->htd', dout, held)
        keyed = rounded(jnp.exp(last[:, None] - running)[:, :, None] * kf)
        state = jnp.exp(last)[:, None, None] * state + jnp.einsum('hsd,hse->hde', keyed, vf)
        return (state, (dout.astype(jnp.bfloat16), grad_q.astype(jnp.bfloat16)))
    zeros = jnp.zeros((HEADS, DH, DH), f32)
    _, (doutb, grad_qb) = lax.scan(forward, zeros, (qb, kb, vb, yb, decays))

    def backward(rear, inputs):
        qry, kys, vls, dout, block_decay = inputs
        running, last, inner = tables(block_decay)
        qf, kf, vf, df = (qry.astype(f32), kys.astype(f32), vls.astype(f32), dout.astype(f32))
        mixing = rounded(inner * jnp.einsum('htd,hsd->hts', qf, kf))
        dmix = rounded(inner * jnp.einsum('hte,hse->hts', df, vf))
        held = rounded(rear)
        ending = jnp.exp(last[:, None] - running)[:, :, None]
        grad_k = jnp.einsum('hts,htd->hsd', dmix, qf) + ending * jnp.einsum('hse,hde->hsd', vf, held)
        grad_v = jnp.einsum('hts,hte->hse', mixing, df) + ending * jnp.einsum('hsd,hde->hse', kf, held)
        queried = rounded(jnp.exp(running)[:, :, None] * qf)
        rear = jnp.exp(last)[:, None, None] * rear + jnp.einsum('htd,hte->hde', queried, df)
        return (rear, (grad_k.astype(jnp.bfloat16), grad_v.astype(jnp.bfloat16)))
    _, (grad_kb, grad_vb) = lax.scan(backward, zeros, (qb, kb, vb, doutb, decays), reverse=True)

    def unblock(x):
        return x.transpose(0, 2, 1, 3).reshape(TOKENS, HEADS * DH)
    return (unblock(grad_qb), unblock(grad_kb), unblock(grad_vb))
```

```python
import functools

import jax
import jax.numpy as jnp
from jax import lax
from jax.experimental import pallas as pl
from jax.experimental.pallas import tpu as pltpu
from jax.sharding import PartitionSpec as P

BLK = 512
TILE = 256
EPS = 1e-06
F32 = jnp.float32
BF16 = jnp.bfloat16
MESH = pl.DeviceIdType.MESH


def dot(a, b, ca=1, cb=0):
    return lax.dot_general(a, b, (((ca,), (cb,)), ((), ())), preferred_element_type=F32)


def flip(x):
    n = x.shape[1]
    eye = lax.broadcasted_iota(jnp.int32, (n, n), 0) == lax.broadcasted_iota(jnp.int32, (n, n), 1)
    return dot(jnp.where(eye, 1.0, 0.0).astype(BF16), x, 1, 1)


def lanes(x, width):
    return jnp.concatenate([x] * (width // x.shape[1]), axis=1)


def kernel(
    n_seq, n_head, features,
    q_hbm, k_hbm, v_hbm, y_hbm, decay_hbm, gain_hbm,
    oq_ref, k_ref, v_ref, gk_ref, gv_ref, end_ref, kept_ref,
    decay_ref, gain_ref, q_ref, y_ref, kt_ref, qt_ref, vt_ref, queried_ref, scaled_ref,
    c_ref, a_ref, col_ref, inner_ref, mix_ref, out_ref, dout_ref,
    state_ref, rear_ref, held_ref, edge_ref,
    tx_ref, rx_ref, stat_ref, stats_ref,
    in_sem, send_sem, recv_sem, hsend_sem, hrecv_sem,
):
    seq = lax.axis_index("seq")
    head = lax.axis_index("head")
    tokens, width = q_ref.shape
    nblk = tokens // BLK
    tiles = BLK // TILE

    barrier = pltpu.get_barrier_semaphore()
    for d in range(1, n_seq):
        pl.semaphore_signal(
            barrier, inc=1, device_id={"seq": lax.rem(seq + d, n_seq)}, device_id_type=MESH
        )
    for d in range(1, n_head):
        pl.semaphore_signal(
            barrier, inc=1, device_id={"head": lax.rem(head + d, n_head)}, device_id_type=MESH
        )

    pairs = [(decay_hbm, decay_ref)]
    for b in range(nblk):
        part = pl.ds(b * BLK, BLK)
        pairs += [(k_hbm.at[part, :], k_ref.at[part, :]), (v_hbm.at[part, :], v_ref.at[part, :])]
    pairs += [(q_hbm, q_ref), (y_hbm, y_ref), (gain_hbm, gain_ref)]
    loads = [
        pltpu.make_async_copy(src, dst, in_sem.at[i]) for i, (src, dst) in enumerate(pairs)
    ]
    for load in loads:
        load.start()

    def span(b, start=0, size=BLK):
        return pl.ds(b * BLK + start, size)

    upper = jnp.where(
        lax.broadcasted_iota(jnp.int32, (BLK, BLK), 0)
        <= lax.broadcasted_iota(jnp.int32, (BLK, BLK), 1),
        1.0, 0.0,
    ).astype(BF16)
    rows = c_ref.shape[0]
    loads[0].wait()
    x = jnp.concatenate(
        [decay_ref[:, b * BLK:(b + 1) * BLK] for b in range(nblk)]
        + ([jnp.zeros((rows - nblk, BLK), F32)] if rows > nblk else []),
        axis=0,
    )
    x1 = x.astype(BF16).astype(F32)
    x2 = (x - x1).astype(BF16).astype(F32)
    x3 = x - x1 - x2
    parts = jnp.concatenate([x1, x2, x3, jnp.zeros_like(x)], axis=0).astype(BF16)
    sums = dot(parts, upper)
    c_all = sums[:rows] + sums[rows:2 * rows] + sums[2 * rows:3 * rows]
    c_ref[...] = c_all
    a_ref[...] = jnp.broadcast_to(c_all[:, BLK - 1:BLK], (rows, width))

    def c_row(b):
        return c_ref[b:b + 1, :]

    def a_row(b):
        return a_ref[b:b + 1, :]

    state = jnp.zeros((width, width), F32)
    own = jnp.zeros((1, width), F32)
    for b in range(nblk):
        loads[1 + 2 * b].wait()
        loads[2 + 2 * b].wait()
        state_ref[b] = state
        kt = flip(k_ref[span(b), :])
        kt_ref[:, span(b)] = kt.astype(BF16)
        ending = jnp.exp(lanes(a_row(b), BLK) - c_row(b))
        piece = dot((ending * kt).astype(BF16), v_ref[span(b), :])
        state = jnp.exp(a_row(b)) * state + piece
        own = own + a_row(b)
    tx_ref[0, :width, :] = state
    tx_ref[0, width:, :] = jnp.broadcast_to(own, (8, width))

    pl.semaphore_wait(barrier, n_seq - 1 + n_head - 1)

    def hop(way, d):
        target = seq + d if way == 0 else seq - d
        return pltpu.make_async_remote_copy(
            src_ref=tx_ref.at[way],
            dst_ref=rx_ref.at[way, d - 1],
            send_sem=send_sem.at[way, d - 1],
            recv_sem=recv_sem.at[way, d - 1],
            device_id={"seq": lax.rem(target + n_seq, n_seq)},
            device_id_type=MESH,
        )

    def reaches(way, d):
        return seq + d < n_seq if way == 0 else seq >= d

    def comes(way, d):
        return reaches(1 - way, d)

    def send(way):
        for d in range(n_seq - 1, 0, -1):
            @pl.when(reaches(way, d))
            def _():
                hop(way, d).start()

    def receive(way):
        edge_ref[:width, :] = jnp.zeros((width, width), F32)
        edge_ref[width:, :] = jnp.zeros((8, width), F32)
        for d in range(1, n_seq):
            @pl.when(comes(way, d))
            def _():
                hop(way, d).wait_recv()
                log = edge_ref[width:width + 1, :]
                edge_ref[:width, :] += jnp.exp(log) * rx_ref[way, d - 1, :width, :]
                edge_ref[width:, :] += rx_ref[way, d - 1, width:, :]
        return edge_ref[:width, :]

    def finish(way):
        for d in range(1, n_seq):
            @pl.when(reaches(way, d))
            def _():
                hop(way, d).wait_send()

    send(0)

    loads[2 * nblk + 1].wait()
    loads[2 * nblk + 3].wait()
    gain_col = jnp.transpose(jnp.broadcast_to(gain_ref[...], (width, width)))
    diagonal = lax.broadcasted_iota(jnp.int32, (TILE, TILE), 0) <= lax.broadcasted_iota(
        jnp.int32, (TILE, TILE), 1
    )
    for b in range(nblk):
        vt_ref[:, span(b)] = flip(v_ref[span(b), :]).astype(BF16)
        qt = flip(q_ref[span(b), :])
        qt_ref[:, span(b)] = qt.astype(BF16)
        queried_ref[:, span(b)] = (jnp.exp(c_row(b)) * qt).astype(BF16)
        col_ref[span(b), :] = jnp.transpose(jnp.broadcast_to(c_row(b), (width, BLK)))
        for i in range(tiles):
            s0 = i * TILE
            rest = BLK - s0
            scores = dot(k_ref[span(b, s0, TILE), :], q_ref[span(b, s0, rest), :], 1, 1)
            diff = c_ref[b:b + 1, s0:] - lanes(col_ref[span(b, s0, TILE), :], rest)
            near = jnp.exp(jnp.where(diagonal, diff[:, :TILE], -jnp.inf))
            inner = near
            if rest > TILE:
                inner = jnp.concatenate([near, jnp.exp(diff[:, TILE:])], axis=1)
            inner_ref[b, s0:s0 + TILE, s0:] = inner
            mix = (inner * scores).astype(BF16)
            mix_ref[b, s0:s0 + TILE, s0:] = mix
            part = dot(vt_ref[:, span(b, s0, TILE)], mix)
            if i == 0:
                out_ref[:, span(b)] = part
            else:
                out_ref[:, span(b, s0, rest)] += part
    loads[2 * nblk + 2].wait()
    for b in range(nblk):
        scaled_ref[:, span(b)] = lanes(gain_col, BLK) * flip(y_ref[span(b), :])

    entering = receive(0)
    before = jnp.zeros((1, width), F32)
    if stat_ref.shape[0] > 2 * nblk:
        stat_ref[...] = jnp.zeros_like(stat_ref)
    for b in range(nblk):
        held = state_ref[b] + jnp.exp(before) * entering
        before = before + a_row(b)
        held_ref[b] = held.astype(BF16)
        carried = dot(jnp.transpose(held).astype(BF16), qt_ref[:, span(b)])
        out = out_ref[:, span(b)] + jnp.exp(c_row(b)) * carried
        out_ref[:, span(b)] = out
        stat_ref[b:b + 1, :] = jnp.sum(out * out, axis=0, keepdims=True)
        stat_ref[nblk + b:nblk + b + 1, :] = jnp.sum(
            out * scaled_ref[:, span(b)], axis=0, keepdims=True
        )

    def share(d):
        return pltpu.make_async_remote_copy(
            src_ref=stat_ref,
            dst_ref=stats_ref.at[d - 1],
            send_sem=hsend_sem.at[d - 1],
            recv_sem=hrecv_sem.at[d - 1],
            device_id={"head": lax.rem(head + d, n_head)},
            device_id_type=MESH,
        )

    for d in range(1, n_head):
        share(d).start()
    total = stat_ref[...]
    for d in range(1, n_head):
        share(d).wait_recv()
        total = total + stats_ref[d - 1]
    inv = lax.rsqrt(total[:nblk] / features + EPS)
    coef = inv * inv * inv * total[nblk:2 * nblk] / features

    rear = jnp.zeros((width, width), F32)
    for b in reversed(range(nblk)):
        dout = (
            inv[b:b + 1] * scaled_ref[:, span(b)] - out_ref[:, span(b)] * coef[b:b + 1]
        ).astype(BF16)
        dout_ref[:, span(b)] = dout
        rear_ref[b] = rear
        rear = jnp.exp(a_row(b)) * rear + dot(queried_ref[:, span(b)], dout, 1, 1)
    tx_ref[1, :width, :] = rear
    tx_ref[1, width:, :] = jnp.broadcast_to(own, (8, width))
    send(1)

    for b in range(nblk):
        grad_q = jnp.exp(c_row(b)) * dot(held_ref[b], dout_ref[:, span(b)])
        halves = [grad_q[:, i * TILE:(i + 1) * TILE] for i in range(tiles)]
        for i in range(tiles):
            s0 = i * TILE
            rest = BLK - s0
            dout = dout_ref[:, span(b, s0, rest)]
            dscores = dot(v_ref[span(b, s0, TILE), :], dout)
            dmix = (inner_ref[b, s0:s0 + TILE, s0:] * dscores).astype(BF16)
            part = dot(kt_ref[:, span(b, s0, TILE)], dmix)
            for j in range(i, tiles):
                halves[j] = halves[j] + part[:, (j - i) * TILE:(j - i + 1) * TILE]
            gk_ref[span(b, s0, TILE), :] = dot(dmix, q_ref[span(b, s0, rest), :])
            gv_ref[span(b, s0, TILE), :] = dot(mix_ref[b, s0:s0 + TILE, s0:], dout, 1, 1)
        for i in range(tiles):
            oq_ref[span(b, i * TILE, TILE), :] = jnp.transpose(halves[i]).astype(BF16)
        end_ref[span(b), :] = jnp.exp(a_row(b) - col_ref[span(b), :])

    leaving = receive(1)
    after = jnp.zeros((1, width), F32)
    for b in reversed(range(nblk)):
        kept_ref[b] = (rear_ref[b] + jnp.exp(after) * leaving).astype(BF16)
        after = after + a_row(b)

    finish(0)
    finish(1)
    for d in range(1, n_head):
        share(d).wait_send()


def closing(
    oq_ref, k_ref, v_ref, gk_ref, gv_ref, end_ref, kept_ref,
    gq_hbm, gk_hbm, gv_hbm,
    ok_ref, ov_ref, out_sem,
):
    tokens = k_ref.shape[0]
    nblk = tokens // BLK

    def span(b):
        return pl.ds(b * BLK, BLK)

    first = pltpu.make_async_copy(oq_ref, gq_hbm, out_sem.at[2 * nblk])
    first.start()
    stores = []
    for b in range(nblk):
        ending = end_ref[span(b), :]
        ok_ref[span(b), :] = (
            gk_ref[span(b), :] + ending * dot(v_ref[span(b), :], kept_ref[b], 1, 1)
        ).astype(BF16)
        ov_ref[span(b), :] = (
            gv_ref[span(b), :] + ending * dot(k_ref[span(b), :], kept_ref[b])
        ).astype(BF16)
        for i, (src, dst) in enumerate(((ok_ref, gk_hbm), (ov_ref, gv_hbm))):
            store = pltpu.make_async_copy(
                src.at[span(b), :], dst.at[span(b), :], out_sem.at[2 * b + i]
            )
            store.start()
            stores.append(store)
    first.wait()
    for store in stores:
        store.wait()


def shards(n_seq, n_head, query, key, value, grad_out, log_decay, gain):
    tokens, width = query.shape
    nblk = tokens // BLK
    features = width * n_head
    rows = -(-nblk // 8) * 8
    srows = -(-2 * nblk // 8) * 8
    big = lambda dtype: pltpu.VMEM((tokens, width), dtype)
    wide = lambda dtype: pltpu.VMEM((width, tokens), dtype)
    shape = jax.ShapeDtypeStruct((tokens, width), BF16)
    hbm = pl.BlockSpec(memory_space=pl.ANY)
    vmem = pl.BlockSpec(memory_space=pltpu.VMEM)
    dma = pltpu.SemaphoreType.DMA
    kept = pltpu.VMEM((nblk, width, width), BF16)
    stay = lambda x: pltpu.with_memory_space_constraint(x, pltpu.HBM)
    middle = pl.pallas_call(
        functools.partial(kernel, n_seq, n_head, features),
        out_shape=(big(BF16), big(BF16), big(BF16), big(F32), big(F32), big(F32), kept),
        in_specs=[pl.BlockSpec(memory_space=pltpu.HBM)] * 6,
        out_specs=(vmem,) * 7,
        scratch_shapes=[
            pltpu.VMEM((1, tokens), F32), pltpu.VMEM((1, width), F32),
            big(BF16), big(BF16),
            wide(BF16), wide(BF16), wide(BF16), wide(BF16), wide(F32),
            pltpu.VMEM((rows, BLK), F32),
            pltpu.VMEM((rows, width), F32),
            big(F32),
            pltpu.VMEM((nblk, BLK, BLK), F32),
            pltpu.VMEM((nblk, BLK, BLK), BF16),
            wide(F32), wide(BF16),
            pltpu.VMEM((nblk, width, width), F32),
            pltpu.VMEM((nblk, width, width), F32),
            pltpu.VMEM((nblk, width, width), BF16),
            pltpu.VMEM((width + 8, width), F32),
            pltpu.VMEM((2, width + 8, width), F32),
            pltpu.VMEM((2, n_seq - 1, width + 8, width), F32),
            pltpu.VMEM((srows, BLK), F32),
            pltpu.VMEM((n_head - 1, srows, BLK), F32),
            dma((2 * nblk + 4,)),
            dma((2, n_seq - 1)), dma((2, n_seq - 1)),
            dma((n_head - 1,)), dma((n_head - 1,)),
        ],
        compiler_params=pltpu.CompilerParams(
            collective_id=0, has_side_effects=True, vmem_limit_bytes=40 << 20
        ),
    )(*map(stay, (query, key, value, grad_out, log_decay, gain.reshape(1, width))))
    return pl.pallas_call(
        closing,
        out_shape=(shape, shape, shape),
        in_specs=[vmem] * 7,
        out_specs=(hbm, hbm, hbm),
        scratch_shapes=[big(BF16), big(BF16), dma((2 * nblk + 1,))],
        compiler_params=pltpu.CompilerParams(vmem_limit_bytes=8 << 20),
    )(*middle)


def solution(mesh):
    return jax.shard_map(
        functools.partial(shards, mesh.shape["seq"], mesh.shape["head"]),
        mesh=mesh,
        in_specs=(
            P("seq", "head"),
            P("seq", "head"),
            P("seq", "head"),
            P("seq", "head"),
            P("head", "seq"),
            P("head"),
        ),
        out_specs=(P("seq", "head"), P("seq", "head"), P("seq", "head")),
        check_vma=False,
    )
```

```python
import functools

import jax
import jax.numpy as jnp
from jax import lax
from jax.experimental import pallas as pl
from jax.experimental.pallas import tpu as pltpu
from jax.sharding import PartitionSpec as P

BLK = 512
TILE = 256
EPS = 1e-06
F32 = jnp.float32
BF16 = jnp.bfloat16
MESH = pl.DeviceIdType.MESH


def dot(a, b, ca=1, cb=0):
    return lax.dot_general(a, b, (((ca,), (cb,)), ((), ())), preferred_element_type=F32)


def flip(x):
    n = x.shape[1]
    eye = lax.broadcasted_iota(jnp.int32, (n, n), 0) == lax.broadcasted_iota(jnp.int32, (n, n), 1)
    return dot(jnp.where(eye, 1.0, 0.0).astype(BF16), x, 1, 1)


def lanes(x, width):
    return jnp.concatenate([x] * (width // x.shape[1]), axis=1)


def kernel(
    n_seq, n_head, features,
    q_hbm, k_hbm, v_hbm, y_hbm, decay_hbm, gain_hbm,
    oq_ref, k_ref, v_ref, gk_ref, gv_ref, end_ref, kept_ref,
    decay_ref, gain_ref, q_ref, y_ref, kt_ref, qt_ref, vt_ref, queried_ref, scaled_ref,
    c_ref, a_ref, col_ref, inner_ref, mix_ref, out_ref, dout_ref,
    state_ref, rear_ref, held_ref, edge_ref,
    tx_ref, rx_ref, stat_ref, stats_ref,
    in_sem, send_sem, recv_sem, hsend_sem, hrecv_sem,
):
    seq = lax.axis_index("seq")
    head = lax.axis_index("head")
    tokens, width = q_ref.shape
    nblk = tokens // BLK
    tiles = BLK // TILE

    barrier = pltpu.get_barrier_semaphore()
    for d in range(1, n_seq):
        pl.semaphore_signal(
            barrier, inc=1, device_id={"seq": lax.rem(seq + d, n_seq)}, device_id_type=MESH
        )
    for d in range(1, n_head):
        pl.semaphore_signal(
            barrier, inc=1, device_id={"head": lax.rem(head + d, n_head)}, device_id_type=MESH
        )

    pairs = [(decay_hbm, decay_ref)]
    for b in range(nblk):
        part = pl.ds(b * BLK, BLK)
        pairs += [(k_hbm.at[part, :], k_ref.at[part, :]), (v_hbm.at[part, :], v_ref.at[part, :])]
    pairs += [(q_hbm, q_ref), (y_hbm, y_ref), (gain_hbm, gain_ref)]
    loads = [
        pltpu.make_async_copy(src, dst, in_sem.at[i]) for i, (src, dst) in enumerate(pairs)
    ]
    for load in loads:
        load.start()

    def span(b, start=0, size=BLK):
        return pl.ds(b * BLK + start, size)

    upper = jnp.where(
        lax.broadcasted_iota(jnp.int32, (BLK, BLK), 0)
        <= lax.broadcasted_iota(jnp.int32, (BLK, BLK), 1),
        1.0, 0.0,
    ).astype(BF16)
    rows = c_ref.shape[0]
    loads[0].wait()
    x = jnp.concatenate(
        [decay_ref[:, b * BLK:(b + 1) * BLK] for b in range(nblk)]
        + ([jnp.zeros((rows - nblk, BLK), F32)] if rows > nblk else []),
        axis=0,
    )
    x1 = x.astype(BF16).astype(F32)
    x2 = (x - x1).astype(BF16).astype(F32)
    x3 = x - x1 - x2
    parts = jnp.concatenate([x1, x2, x3, jnp.zeros_like(x)], axis=0).astype(BF16)
    sums = dot(parts, upper)
    c_all = sums[:rows] + sums[rows:2 * rows] + sums[2 * rows:3 * rows]
    c_ref[...] = c_all
    a_ref[...] = jnp.broadcast_to(c_all[:, BLK - 1:BLK], (rows, width))

    def c_row(b):
        return c_ref[b:b + 1, :]

    def a_row(b):
        return a_ref[b:b + 1, :]

    state = jnp.zeros((width, width), F32)
    own = jnp.zeros((1, width), F32)
    for b in range(nblk):
        loads[1 + 2 * b].wait()
        loads[2 + 2 * b].wait()
        state_ref[b] = state
        kt = flip(k_ref[span(b), :])
        kt_ref[:, span(b)] = kt.astype(BF16)
        ending = jnp.exp(lanes(a_row(b), BLK) - c_row(b))
        piece = dot((ending * kt).astype(BF16), v_ref[span(b), :])
        state = jnp.exp(a_row(b)) * state + piece
        own = own + a_row(b)
    tx_ref[0, :width, :] = state
    tx_ref[0, width:, :] = jnp.broadcast_to(own, (8, width))

    pl.semaphore_wait(barrier, n_seq - 1 + n_head - 1)

    def hop(way, d):
        target = seq + d if way == 0 else seq - d
        return pltpu.make_async_remote_copy(
            src_ref=tx_ref.at[way],
            dst_ref=rx_ref.at[way, d - 1],
            send_sem=send_sem.at[way, d - 1],
            recv_sem=recv_sem.at[way, d - 1],
            device_id={"seq": lax.rem(target + n_seq, n_seq)},
            device_id_type=MESH,
        )

    def reaches(way, d):
        return seq + d < n_seq if way == 0 else seq >= d

    def comes(way, d):
        return reaches(1 - way, d)

    def send(way):
        for d in range(1, n_seq) if way == 0 else range(n_seq - 1, 0, -1):
            @pl.when(reaches(way, d))
            def _():
                hop(way, d).start()

    def receive(way):
        edge_ref[:width, :] = jnp.zeros((width, width), F32)
        edge_ref[width:, :] = jnp.zeros((8, width), F32)
        for d in range(1, n_seq):
            @pl.when(comes(way, d))
            def _():
                hop(way, d).wait_recv()
                log = edge_ref[width:width + 1, :]
                edge_ref[:width, :] += jnp.exp(log) * rx_ref[way, d - 1, :width, :]
                edge_ref[width:, :] += rx_ref[way, d - 1, width:, :]
        return edge_ref[:width, :]

    def finish(way):
        for d in range(1, n_seq):
            @pl.when(reaches(way, d))
            def _():
                hop(way, d).wait_send()

    send(0)

    loads[2 * nblk + 1].wait()
    loads[2 * nblk + 3].wait()
    gain_col = jnp.transpose(jnp.broadcast_to(gain_ref[...], (width, width)))
    diagonal = lax.broadcasted_iota(jnp.int32, (TILE, TILE), 0) <= lax.broadcasted_iota(
        jnp.int32, (TILE, TILE), 1
    )
    for b in range(nblk):
        vt_ref[:, span(b)] = flip(v_ref[span(b), :]).astype(BF16)
        qt = flip(q_ref[span(b), :])
        qt_ref[:, span(b)] = qt.astype(BF16)
        queried_ref[:, span(b)] = (jnp.exp(c_row(b)) * qt).astype(BF16)
        col_ref[span(b), :] = jnp.transpose(jnp.broadcast_to(c_row(b), (width, BLK)))
        for i in range(tiles):
            s0 = i * TILE
            rest = BLK - s0
            scores = dot(k_ref[span(b, s0, TILE), :], q_ref[span(b, s0, rest), :], 1, 1)
            diff = c_ref[b:b + 1, s0:] - lanes(col_ref[span(b, s0, TILE), :], rest)
            near = jnp.exp(jnp.where(diagonal, diff[:, :TILE], -jnp.inf))
            inner = near
            if rest > TILE:
                inner = jnp.concatenate([near, jnp.exp(diff[:, TILE:])], axis=1)
            inner_ref[b, s0:s0 + TILE, s0:] = inner
            mix = (inner * scores).astype(BF16)
            mix_ref[b, s0:s0 + TILE, s0:] = mix
            part = dot(vt_ref[:, span(b, s0, TILE)], mix)
            if i == 0:
                out_ref[:, span(b)] = part
            else:
                out_ref[:, span(b, s0, rest)] += part
    loads[2 * nblk + 2].wait()
    for b in range(nblk):
        scaled_ref[:, span(b)] = lanes(gain_col, BLK) * flip(y_ref[span(b), :])

    entering = receive(0)
    before = jnp.zeros((1, width), F32)
    if stat_ref.shape[0] > 2 * nblk:
        stat_ref[...] = jnp.zeros_like(stat_ref)
    for b in range(nblk):
        held = state_ref[b] + jnp.exp(before) * entering
        before = before + a_row(b)
        held_ref[b] = held.astype(BF16)
        carried = dot(jnp.transpose(held).astype(BF16), qt_ref[:, span(b)])
        out = out_ref[:, span(b)] + jnp.exp(c_row(b)) * carried
        out_ref[:, span(b)] = out
        stat_ref[b:b + 1, :] = jnp.sum(out * out, axis=0, keepdims=True)
        stat_ref[nblk + b:nblk + b + 1, :] = jnp.sum(
            out * scaled_ref[:, span(b)], axis=0, keepdims=True
        )

    def share(d):
        return pltpu.make_async_remote_copy(
            src_ref=stat_ref,
            dst_ref=stats_ref.at[d - 1],
            send_sem=hsend_sem.at[d - 1],
            recv_sem=hrecv_sem.at[d - 1],
            device_id={"head": lax.rem(head + d, n_head)},
            device_id_type=MESH,
        )

    for d in range(1, n_head):
        share(d).start()
    total = stat_ref[...]
    for d in range(1, n_head):
        share(d).wait_recv()
        total = total + stats_ref[d - 1]
    inv = lax.rsqrt(total[:nblk] / features + EPS)
    coef = inv * inv * inv * total[nblk:2 * nblk] / features

    rear = jnp.zeros((width, width), F32)
    for b in reversed(range(nblk)):
        dout = (
            inv[b:b + 1] * scaled_ref[:, span(b)] - out_ref[:, span(b)] * coef[b:b + 1]
        ).astype(BF16)
        dout_ref[:, span(b)] = dout
        rear_ref[b] = rear
        rear = jnp.exp(a_row(b)) * rear + dot(queried_ref[:, span(b)], dout, 1, 1)
    tx_ref[1, :width, :] = rear
    tx_ref[1, width:, :] = jnp.broadcast_to(own, (8, width))
    send(1)

    for b in range(nblk):
        grad_q = jnp.exp(c_row(b)) * dot(held_ref[b], dout_ref[:, span(b)])
        halves = [grad_q[:, i * TILE:(i + 1) * TILE] for i in range(tiles)]
        for i in range(tiles):
            s0 = i * TILE
            rest = BLK - s0
            dout = dout_ref[:, span(b, s0, rest)]
            dscores = dot(v_ref[span(b, s0, TILE), :], dout)
            dmix = (inner_ref[b, s0:s0 + TILE, s0:] * dscores).astype(BF16)
            part = dot(kt_ref[:, span(b, s0, TILE)], dmix)
            for j in range(i, tiles):
                halves[j] = halves[j] + part[:, (j - i) * TILE:(j - i + 1) * TILE]
            gk_ref[span(b, s0, TILE), :] = dot(dmix, q_ref[span(b, s0, rest), :])
            gv_ref[span(b, s0, TILE), :] = dot(mix_ref[b, s0:s0 + TILE, s0:], dout, 1, 1)
        for i in range(tiles):
            oq_ref[span(b, i * TILE, TILE), :] = jnp.transpose(halves[i]).astype(BF16)
        end_ref[span(b), :] = jnp.exp(a_row(b) - col_ref[span(b), :])

    leaving = receive(1)
    after = jnp.zeros((1, width), F32)
    for b in reversed(range(nblk)):
        kept_ref[b] = (rear_ref[b] + jnp.exp(after) * leaving).astype(BF16)
        after = after + a_row(b)

    finish(0)
    finish(1)
    for d in range(1, n_head):
        share(d).wait_send()


def closing(
    oq_ref, k_ref, v_ref, gk_ref, gv_ref, end_ref, kept_ref,
    gq_hbm, gk_hbm, gv_hbm,
    ok_ref, ov_ref, out_sem,
):
    tokens = k_ref.shape[0]
    nblk = tokens // BLK

    def span(b):
        return pl.ds(b * BLK, BLK)

    first = pltpu.make_async_copy(oq_ref, gq_hbm, out_sem.at[2 * nblk])
    first.start()
    stores = []
    for b in range(nblk):
        ending = end_ref[span(b), :]
        ok_ref[span(b), :] = (
            gk_ref[span(b), :] + ending * dot(v_ref[span(b), :], kept_ref[b], 1, 1)
        ).astype(BF16)
        ov_ref[span(b), :] = (
            gv_ref[span(b), :] + ending * dot(k_ref[span(b), :], kept_ref[b])
        ).astype(BF16)
        for i, (src, dst) in enumerate(((ok_ref, gk_hbm), (ov_ref, gv_hbm))):
            store = pltpu.make_async_copy(
                src.at[span(b), :], dst.at[span(b), :], out_sem.at[2 * b + i]
            )
            store.start()
            stores.append(store)
    first.wait()
    for store in stores:
        store.wait()


def shards(n_seq, n_head, query, key, value, grad_out, log_decay, gain):
    tokens, width = query.shape
    nblk = tokens // BLK
    features = width * n_head
    rows = -(-nblk // 8) * 8
    srows = -(-2 * nblk // 8) * 8
    big = lambda dtype: pltpu.VMEM((tokens, width), dtype)
    wide = lambda dtype: pltpu.VMEM((width, tokens), dtype)
    shape = jax.ShapeDtypeStruct((tokens, width), BF16)
    hbm = pl.BlockSpec(memory_space=pl.ANY)
    vmem = pl.BlockSpec(memory_space=pltpu.VMEM)
    dma = pltpu.SemaphoreType.DMA
    kept = pltpu.VMEM((nblk, width, width), BF16)
    stay = lambda x: pltpu.with_memory_space_constraint(x, pltpu.HBM)
    middle = pl.pallas_call(
        functools.partial(kernel, n_seq, n_head, features),
        out_shape=(big(BF16), big(BF16), big(BF16), big(F32), big(F32), big(F32), kept),
        in_specs=[pl.BlockSpec(memory_space=pltpu.HBM)] * 6,
        out_specs=(vmem,) * 7,
        scratch_shapes=[
            pltpu.VMEM((1, tokens), F32), pltpu.VMEM((1, width), F32),
            big(BF16), big(BF16),
            wide(BF16), wide(BF16), wide(BF16), wide(BF16), wide(F32),
            pltpu.VMEM((rows, BLK), F32),
            pltpu.VMEM((rows, width), F32),
            big(F32),
            pltpu.VMEM((nblk, BLK, BLK), F32),
            pltpu.VMEM((nblk, BLK, BLK), BF16),
            wide(F32), wide(BF16),
            pltpu.VMEM((nblk, width, width), F32),
            pltpu.VMEM((nblk, width, width), F32),
            pltpu.VMEM((nblk, width, width), BF16),
            pltpu.VMEM((width + 8, width), F32),
            pltpu.VMEM((2, width + 8, width), F32),
            pltpu.VMEM((2, n_seq - 1, width + 8, width), F32),
            pltpu.VMEM((srows, BLK), F32),
            pltpu.VMEM((n_head - 1, srows, BLK), F32),
            dma((2 * nblk + 4,)),
            dma((2, n_seq - 1)), dma((2, n_seq - 1)),
            dma((n_head - 1,)), dma((n_head - 1,)),
        ],
        compiler_params=pltpu.CompilerParams(
            collective_id=0, has_side_effects=True, vmem_limit_bytes=40 << 20
        ),
    )(*map(stay, (query, key, value, grad_out, log_decay, gain.reshape(1, width))))
    return pl.pallas_call(
        closing,
        out_shape=(shape, shape, shape),
        in_specs=[vmem] * 7,
        out_specs=(hbm, hbm, hbm),
        scratch_shapes=[big(BF16), big(BF16), dma((2 * nblk + 1,))],
        compiler_params=pltpu.CompilerParams(vmem_limit_bytes=8 << 20),
    )(*middle)


def solution(mesh):
    return jax.shard_map(
        functools.partial(shards, mesh.shape["seq"], mesh.shape["head"]),
        mesh=mesh,
        in_specs=(
            P("seq", "head"),
            P("seq", "head"),
            P("seq", "head"),
            P("seq", "head"),
            P("head", "seq"),
            P("head"),
        ),
        out_specs=(P("seq", "head"), P("seq", "head"), P("seq", "head")),
        check_vma=False,
    )
```

```python
import functools

import jax
import jax.numpy as jnp
from jax import lax
from jax.experimental import pallas as pl
from jax.experimental.pallas import tpu as pltpu
from jax.sharding import PartitionSpec as P

BLK = 512
TILE = 256
EPS = 1e-06
F32 = jnp.float32
BF16 = jnp.bfloat16
MESH = pl.DeviceIdType.MESH


def dot(a, b, ca=1, cb=0):
    return lax.dot_general(a, b, (((ca,), (cb,)), ((), ())), preferred_element_type=F32)


def flip(x):
    n = x.shape[1]
    eye = lax.broadcasted_iota(jnp.int32, (n, n), 0) == lax.broadcasted_iota(jnp.int32, (n, n), 1)
    return dot(jnp.where(eye, 1.0, 0.0).astype(BF16), x, 1, 1)


def lanes(x, width):
    return jnp.concatenate([x] * (width // x.shape[1]), axis=1)


def kernel(
    n_seq, n_head, features,
    q_hbm, k_hbm, v_hbm, y_hbm, decay_hbm, gain_hbm,
    oq_ref, k_ref, v_ref, gk_ref, gv_ref, end_ref, kept_ref,
    decay_ref, gain_ref, q_ref, y_ref, kt_ref, qt_ref, vt_ref, queried_ref, scaled_ref,
    c_ref, a_ref, col_ref, inner_ref, mix_ref, out_ref, dout_ref,
    state_ref, rear_ref, held_ref, edge_ref,
    tx_ref, rx_ref, back_ref, rear_rx_ref, scale_ref, stat_ref, stats_ref,
    in_sem, send_sem, recv_sem, hsend_sem, hrecv_sem,
):
    seq = lax.axis_index("seq")
    head = lax.axis_index("head")
    tokens, width = q_ref.shape
    nblk = tokens // BLK
    tiles = BLK // TILE

    barrier = pltpu.get_barrier_semaphore()
    for d in range(1, n_seq):
        pl.semaphore_signal(
            barrier, inc=1, device_id={"seq": lax.rem(seq + d, n_seq)}, device_id_type=MESH
        )
    for d in range(1, n_head):
        pl.semaphore_signal(
            barrier, inc=1, device_id={"head": lax.rem(head + d, n_head)}, device_id_type=MESH
        )

    pairs = [(decay_hbm, decay_ref)]
    for src, dst in ((k_hbm, k_ref), (v_hbm, v_ref)):
        for b in range(nblk):
            part = pl.ds(b * BLK, BLK)
            pairs.append((src.at[part, :], dst.at[part, :]))
    pairs += [(q_hbm, q_ref), (y_hbm, y_ref), (gain_hbm, gain_ref)]
    loads = [
        pltpu.make_async_copy(src, dst, in_sem.at[i]) for i, (src, dst) in enumerate(pairs)
    ]
    for load in loads:
        load.start()

    def span(b, start=0, size=BLK):
        return pl.ds(b * BLK + start, size)

    rows = c_ref.shape[0]
    upper = jnp.where(
        lax.broadcasted_iota(jnp.int32, (width, width), 0)
        <= lax.broadcasted_iota(jnp.int32, (width, width), 1),
        1.0, 0.0,
    ).astype(BF16)
    pieces = BLK // width
    pad = [jnp.zeros((rows - nblk, width), F32)] if rows > nblk else []
    loads[0].wait()
    for b in range(nblk):
        loads[1 + b].wait()
        loads[1 + nblk + b].wait()
    x = jnp.concatenate(
        sum(
            (
                [
                    decay_ref[:, b * BLK + j * width:b * BLK + (j + 1) * width]
                    for b in range(nblk)
                ]
                + pad
                for j in range(pieces)
            ),
            [],
        ),
        axis=0,
    )
    x1 = x.astype(BF16).astype(F32)
    x2 = (x - x1).astype(BF16).astype(F32)
    x3 = x - x1 - x2
    sums = dot(jnp.concatenate([x1, x2, x3], axis=0).astype(BF16), upper)
    size = pieces * rows
    sums = sums[:size] + sums[size:2 * size] + sums[2 * size:]
    total = jnp.zeros((rows, width), F32)
    for j in range(pieces):
        piece = sums[j * rows:(j + 1) * rows]
        c_ref[:, j * width:(j + 1) * width] = piece + total
        total = total + jnp.broadcast_to(piece[:, width - 1:], (rows, width))
    a_ref[...] = total

    def c_row(b):
        return c_ref[b:b + 1, :]

    def a_row(b):
        return a_ref[b:b + 1, :]

    keyed = []
    for b in range(nblk):
        kt = flip(k_ref[span(b), :])
        kt_ref[:, span(b)] = kt.astype(BF16)
        ending = jnp.exp(lanes(a_row(b), BLK) - c_row(b))
        keyed.append((ending * kt).astype(BF16))
    state = jnp.zeros((width, width), F32)
    own = jnp.zeros((1, width), F32)
    for b in range(nblk):
        state_ref[b] = state
        state = jnp.exp(a_row(b)) * state + dot(keyed[b], v_ref[span(b), :])
        own = own + a_row(b)
    tx_ref[:width, :] = state
    tx_ref[width:, :] = jnp.broadcast_to(own, (8, width))

    pl.semaphore_wait(barrier, n_seq - 1 + n_head - 1)

    def hop(way, d):
        if way == 0:
            head_rows = pl.ds(0, width + 1)
            target, src, dst = seq + d, tx_ref.at[head_rows, :], rx_ref.at[d - 1, head_rows, :]
        else:
            target, src, dst = seq - d, back_ref.at[d - 1], rear_rx_ref.at[d - 1]
        return pltpu.make_async_remote_copy(
            src_ref=src,
            dst_ref=dst,
            send_sem=send_sem.at[way, d - 1],
            recv_sem=recv_sem.at[way, d - 1],
            device_id={"seq": lax.rem(target + n_seq, n_seq)},
            device_id_type=MESH,
        )

    def reaches(way, d):
        return seq + d < n_seq if way == 0 else seq >= d

    def comes(way, d):
        return reaches(1 - way, d)

    def receive():
        edge_ref[:width, :] = jnp.zeros((width, width), F32)
        edge_ref[width:, :] = jnp.zeros((8, width), F32)
        for d in range(1, n_seq):
            @pl.when(comes(0, d))
            def _():
                hop(0, d).wait_recv()
                log = edge_ref[width:width + 1, :]
                scale_ref[d - 1:d, :] = log
                edge_ref[:width, :] += jnp.exp(log) * rx_ref[d - 1, :width, :]
                edge_ref[width:width + 1, :] += rx_ref[d - 1, width:width + 1, :]
        return edge_ref[:width, :]

    def receive_back():
        edge_ref[:width, :] = jnp.zeros((width, width), F32)
        for d in range(1, n_seq):
            @pl.when(comes(1, d))
            def _():
                hop(1, d).wait_recv()
                edge_ref[:width, :] += rear_rx_ref[d - 1]
        return edge_ref[:width, :]

    def send_back(far):
        for d in range(n_seq - 1, 0, -1):
            @pl.when(seq == d if far else seq > d)
            def _():
                back_ref[d - 1] = jnp.exp(scale_ref[d - 1:d, :]) * rear_ref[nblk]
                hop(1, d).start()

    def finish(way):
        for d in range(1, n_seq):
            @pl.when(reaches(way, d))
            def _():
                hop(way, d).wait_send()

    for d in range(1, n_seq):
        @pl.when(reaches(0, d))
        def _():
            hop(0, d).start()

    loads[2 * nblk + 1].wait()
    loads[2 * nblk + 3].wait()
    gain_col = jnp.transpose(jnp.broadcast_to(gain_ref[...], (width, width)))
    diagonal = lax.broadcasted_iota(jnp.int32, (TILE, TILE), 0) <= lax.broadcasted_iota(
        jnp.int32, (TILE, TILE), 1
    )
    for b in range(nblk):
        vt_ref[:, span(b)] = flip(v_ref[span(b), :]).astype(BF16)
        qt = flip(q_ref[span(b), :])
        qt_ref[:, span(b)] = qt.astype(BF16)
        queried_ref[:, span(b)] = (jnp.exp(c_row(b)) * qt).astype(BF16)
        col_ref[span(b), :] = jnp.transpose(jnp.broadcast_to(c_row(b), (width, BLK)))
        for i in range(tiles):
            s0 = i * TILE
            rest = BLK - s0
            scores = dot(k_ref[span(b, s0, TILE), :], q_ref[span(b, s0, rest), :], 1, 1)
            diff = c_ref[b:b + 1, s0:] - lanes(col_ref[span(b, s0, TILE), :], rest)
            near = jnp.exp(jnp.where(diagonal, diff[:, :TILE], -jnp.inf))
            inner = near
            if rest > TILE:
                inner = jnp.concatenate([near, jnp.exp(diff[:, TILE:])], axis=1)
            inner_ref[b, s0:s0 + TILE, s0:] = inner
            mix = (inner * scores).astype(BF16)
            mix_ref[b, s0:s0 + TILE, s0:] = mix
            part = dot(vt_ref[:, span(b, s0, TILE)], mix)
            if i == 0:
                out_ref[:, span(b)] = part
            else:
                out_ref[:, span(b, s0, rest)] += part
    loads[2 * nblk + 2].wait()
    for b in range(nblk):
        scaled_ref[:, span(b)] = lanes(gain_col, BLK) * flip(y_ref[span(b), :])

    entering = receive()
    before = jnp.zeros((1, width), F32)
    if stat_ref.shape[0] > 2 * nblk:
        stat_ref[...] = jnp.zeros_like(stat_ref)
    for b in range(nblk):
        held = state_ref[b] + jnp.exp(before) * entering
        before = before + a_row(b)
        held_ref[b] = held.astype(BF16)
        carried = dot(jnp.transpose(held).astype(BF16), qt_ref[:, span(b)])
        out = out_ref[:, span(b)] + jnp.exp(c_row(b)) * carried
        out_ref[:, span(b)] = out
        stat_ref[b:b + 1, :] = jnp.sum(out * out, axis=0, keepdims=True)
        stat_ref[nblk + b:nblk + b + 1, :] = jnp.sum(
            out * scaled_ref[:, span(b)], axis=0, keepdims=True
        )

    def share(d):
        return pltpu.make_async_remote_copy(
            src_ref=stat_ref,
            dst_ref=stats_ref.at[d - 1],
            send_sem=hsend_sem.at[d - 1],
            recv_sem=hrecv_sem.at[d - 1],
            device_id={"head": lax.rem(head + d, n_head)},
            device_id_type=MESH,
        )

    for d in range(1, n_head):
        share(d).start()
    total = stat_ref[...]
    for d in range(1, n_head):
        share(d).wait_recv()
        total = total + stats_ref[d - 1]
    inv = lax.rsqrt(total[:nblk] / features + EPS)
    coef = inv * inv * inv * total[nblk:2 * nblk] / features

    rear = jnp.zeros((width, width), F32)
    for b in reversed(range(nblk)):
        dout = (
            inv[b:b + 1] * scaled_ref[:, span(b)] - out_ref[:, span(b)] * coef[b:b + 1]
        ).astype(BF16)
        dout_ref[:, span(b)] = dout
        rear_ref[b] = rear
        rear = jnp.exp(a_row(b)) * rear + dot(queried_ref[:, span(b)], dout, 1, 1)
    rear_ref[nblk] = rear
    send_back(True)

    for b in range(nblk):
        grad_q = jnp.exp(c_row(b)) * dot(held_ref[b], dout_ref[:, span(b)])
        halves = [grad_q[:, i * TILE:(i + 1) * TILE] for i in range(tiles)]
        for i in range(tiles):
            s0 = i * TILE
            rest = BLK - s0
            dout = dout_ref[:, span(b, s0, rest)]
            dscores = dot(v_ref[span(b, s0, TILE), :], dout)
            dmix = (inner_ref[b, s0:s0 + TILE, s0:] * dscores).astype(BF16)
            part = dot(kt_ref[:, span(b, s0, TILE)], dmix)
            for j in range(i, tiles):
                halves[j] = halves[j] + part[:, (j - i) * TILE:(j - i + 1) * TILE]
            gk_ref[span(b, s0, TILE), :] = dot(dmix, q_ref[span(b, s0, rest), :])
            gv_ref[span(b, s0, TILE), :] = dot(mix_ref[b, s0:s0 + TILE, s0:], dout, 1, 1)
        for i in range(tiles):
            oq_ref[span(b, i * TILE, TILE), :] = jnp.transpose(halves[i]).astype(BF16)
        end_ref[span(b), :] = jnp.exp(a_row(b) - col_ref[span(b), :])
        if b == min(1, nblk - 1):
            send_back(False)

    leaving = receive_back()
    after = jnp.zeros((1, width), F32)
    for b in reversed(range(nblk)):
        kept_ref[b] = (rear_ref[b] + jnp.exp(after) * leaving).astype(BF16)
        after = after + a_row(b)

    finish(0)
    finish(1)
    for d in range(1, n_head):
        share(d).wait_send()


def closing(
    oq_ref, k_ref, v_ref, gk_ref, gv_ref, end_ref, kept_ref,
    gq_hbm, gk_hbm, gv_hbm,
    ok_ref, ov_ref, out_sem,
):
    tokens = k_ref.shape[0]
    nblk = tokens // BLK

    def span(b):
        return pl.ds(b * BLK, BLK)

    first = pltpu.make_async_copy(oq_ref, gq_hbm, out_sem.at[2 * nblk])
    first.start()
    stores = []
    for b in range(nblk):
        ending = end_ref[span(b), :]
        ok_ref[span(b), :] = (
            gk_ref[span(b), :] + ending * dot(v_ref[span(b), :], kept_ref[b], 1, 1)
        ).astype(BF16)
        ov_ref[span(b), :] = (
            gv_ref[span(b), :] + ending * dot(k_ref[span(b), :], kept_ref[b])
        ).astype(BF16)
        for i, (src, dst) in enumerate(((ok_ref, gk_hbm), (ov_ref, gv_hbm))):
            store = pltpu.make_async_copy(
                src.at[span(b), :], dst.at[span(b), :], out_sem.at[2 * b + i]
            )
            store.start()
            stores.append(store)
    first.wait()
    for store in stores:
        store.wait()


def shards(n_seq, n_head, query, key, value, grad_out, log_decay, gain):
    tokens, width = query.shape
    nblk = tokens // BLK
    features = width * n_head
    rows = -(-nblk // 8) * 8
    srows = -(-2 * nblk // 8) * 8
    big = lambda dtype: pltpu.VMEM((tokens, width), dtype)
    wide = lambda dtype: pltpu.VMEM((width, tokens), dtype)
    shape = jax.ShapeDtypeStruct((tokens, width), BF16)
    hbm = pl.BlockSpec(memory_space=pl.ANY)
    vmem = pl.BlockSpec(memory_space=pltpu.VMEM)
    dma = pltpu.SemaphoreType.DMA
    kept = pltpu.VMEM((nblk, width, width), BF16)
    stay = lambda x: pltpu.with_memory_space_constraint(x, pltpu.HBM)
    middle = pl.pallas_call(
        functools.partial(kernel, n_seq, n_head, features),
        out_shape=(big(BF16), big(BF16), big(BF16), big(F32), big(F32), big(F32), kept),
        in_specs=[pl.BlockSpec(memory_space=pltpu.HBM)] * 6,
        out_specs=(vmem,) * 7,
        scratch_shapes=[
            pltpu.VMEM((1, tokens), F32), pltpu.VMEM((1, width), F32),
            big(BF16), big(BF16),
            wide(BF16), wide(BF16), wide(BF16), wide(BF16), wide(F32),
            pltpu.VMEM((rows, BLK), F32),
            pltpu.VMEM((rows, width), F32),
            big(F32),
            pltpu.VMEM((nblk, BLK, BLK), F32),
            pltpu.VMEM((nblk, BLK, BLK), BF16),
            wide(F32), wide(BF16),
            pltpu.VMEM((nblk, width, width), F32),
            pltpu.VMEM((nblk + 1, width, width), F32),
            pltpu.VMEM((nblk, width, width), BF16),
            pltpu.VMEM((width + 8, width), F32),
            pltpu.VMEM((width + 8, width), F32),
            pltpu.VMEM((n_seq - 1, width + 8, width), F32),
            pltpu.VMEM((n_seq - 1, width, width), F32),
            pltpu.VMEM((n_seq - 1, width, width), F32),
            pltpu.VMEM((n_seq, width), F32),
            pltpu.VMEM((srows, BLK), F32),
            pltpu.VMEM((n_head - 1, srows, BLK), F32),
            dma((2 * nblk + 4,)),
            dma((2, n_seq - 1)), dma((2, n_seq - 1)),
            dma((n_head - 1,)), dma((n_head - 1,)),
        ],
        compiler_params=pltpu.CompilerParams(
            collective_id=0, has_side_effects=True, vmem_limit_bytes=40 << 20
        ),
    )(*map(stay, (query, key, value, grad_out, log_decay, gain.reshape(1, width))))
    return pl.pallas_call(
        closing,
        out_shape=(shape, shape, shape),
        in_specs=[vmem] * 7,
        out_specs=(hbm, hbm, hbm),
        scratch_shapes=[big(BF16), big(BF16), dma((2 * nblk + 1,))],
        compiler_params=pltpu.CompilerParams(vmem_limit_bytes=8 << 20),
    )(*middle)


def solution(mesh):
    return jax.shard_map(
        functools.partial(shards, mesh.shape["seq"], mesh.shape["head"]),
        mesh=mesh,
        in_specs=(
            P("seq", "head"),
            P("seq", "head"),
            P("seq", "head"),
            P("seq", "head"),
            P("head", "seq"),
            P("head"),
        ),
        out_specs=(P("seq", "head"), P("seq", "head"), P("seq", "head")),
        check_vma=False,
    )
```

```python
import functools

import jax
import jax.numpy as jnp
from jax import lax
from jax.experimental import pallas as pl
from jax.experimental.pallas import tpu as pltpu
from jax.sharding import PartitionSpec as P

BLK = 512
TILE = 256
EPS = 1e-06
F32 = jnp.float32
BF16 = jnp.bfloat16
MESH = pl.DeviceIdType.MESH


def dot(a, b, ca=1, cb=0):
    return lax.dot_general(a, b, (((ca,), (cb,)), ((), ())), preferred_element_type=F32)


def flip(x):
    n = x.shape[1]
    eye = lax.broadcasted_iota(jnp.int32, (n, n), 0) == lax.broadcasted_iota(jnp.int32, (n, n), 1)
    return dot(jnp.where(eye, 1.0, 0.0).astype(BF16), x, 1, 1)


def lanes(x, width):
    return jnp.concatenate([x] * (width // x.shape[1]), axis=1)


def kernel(
    n_seq, n_head, features,
    q_hbm, k_hbm, v_hbm, y_hbm, decay_hbm, gain_hbm,
    oq_ref, k_ref, v_ref, gk_ref, gv_ref, end_ref, kept_ref,
    decay_ref, gain_ref, q_ref, y_ref, kt_ref, qt_ref, vt_ref, queried_ref, scaled_ref,
    c_ref, a_ref, col_ref, inner_ref, mix_ref, out_ref, dout_ref,
    state_ref, rear_ref, held_ref, edge_ref,
    tx_ref, rx_ref, back_ref, rear_rx_ref, scale_ref, flipped_ref, scales_ref, stat_ref, stats_ref,
    in_sem, send_sem, recv_sem, hsend_sem, hrecv_sem,
):
    seq = lax.axis_index("seq")
    head = lax.axis_index("head")
    tokens, width = q_ref.shape
    nblk = tokens // BLK
    tiles = BLK // TILE

    barrier = pltpu.get_barrier_semaphore()
    for d in range(1, n_seq):
        pl.semaphore_signal(
            barrier, inc=1, device_id={"seq": lax.rem(seq + d, n_seq)}, device_id_type=MESH
        )
    for d in range(1, n_head):
        pl.semaphore_signal(
            barrier, inc=1, device_id={"head": lax.rem(head + d, n_head)}, device_id_type=MESH
        )

    pairs = (
        (decay_hbm, decay_ref), (k_hbm, k_ref), (v_hbm, v_ref), (q_hbm, q_ref), (y_hbm, y_ref),
        (gain_hbm, gain_ref),
    )
    loads = [
        pltpu.make_async_copy(src, dst, in_sem.at[i]) for i, (src, dst) in enumerate(pairs)
    ]
    for load in loads:
        load.start()

    def span(b, start=0, size=BLK):
        return pl.ds(b * BLK + start, size)

    rows = c_ref.shape[0]
    upper = jnp.where(
        lax.broadcasted_iota(jnp.int32, (width, width), 0)
        <= lax.broadcasted_iota(jnp.int32, (width, width), 1),
        1.0, 0.0,
    ).astype(BF16)
    pieces = BLK // width
    pad = [jnp.zeros((rows - nblk, width), F32)] if rows > nblk else []
    loads[0].wait()
    loads[1].wait()
    loads[2].wait()
    x = jnp.concatenate(
        sum(
            (
                [
                    decay_ref[:, b * BLK + j * width:b * BLK + (j + 1) * width]
                    for b in range(nblk)
                ]
                + pad
                for j in range(pieces)
            ),
            [],
        ),
        axis=0,
    )
    x1 = x.astype(BF16).astype(F32)
    x2 = (x - x1).astype(BF16).astype(F32)
    x3 = x - x1 - x2
    sums = dot(jnp.concatenate([x1, x2, x3], axis=0).astype(BF16), upper)
    size = pieces * rows
    sums = sums[:size] + sums[size:2 * size] + sums[2 * size:]
    total = jnp.zeros((rows, width), F32)
    for j in range(pieces):
        piece = sums[j * rows:(j + 1) * rows]
        c_ref[:, j * width:(j + 1) * width] = piece + total
        total = total + jnp.broadcast_to(piece[:, width - 1:], (rows, width))
    a_ref[...] = total

    def c_row(b):
        return c_ref[b:b + 1, :]

    def a_row(b):
        return a_ref[b:b + 1, :]

    keyed = []
    for b in range(nblk):
        kt = flip(k_ref[span(b), :])
        kt_ref[:, span(b)] = kt.astype(BF16)
        ending = jnp.exp(lanes(a_row(b), BLK) - c_row(b))
        keyed.append((ending * kt).astype(BF16))
    state = jnp.zeros((width, width), F32)
    own = jnp.zeros((1, width), F32)
    for b in range(nblk):
        state_ref[b] = state
        state = jnp.exp(a_row(b)) * state + dot(keyed[b], v_ref[span(b), :])
        own = own + a_row(b)
    tx_ref[:width, :] = state
    tx_ref[width:, :] = jnp.broadcast_to(own, (8, width))

    pl.semaphore_wait(barrier, n_seq - 1 + n_head - 1)

    def hop(way, d):
        if way == 0:
            head_rows = pl.ds(0, width + 1)
            target, src, dst = seq + d, tx_ref.at[head_rows, :], rx_ref.at[d - 1, head_rows, :]
        else:
            target, src, dst = seq - d, back_ref.at[d - 1], rear_rx_ref.at[d - 1]
        return pltpu.make_async_remote_copy(
            src_ref=src,
            dst_ref=dst,
            send_sem=send_sem.at[way, d - 1],
            recv_sem=recv_sem.at[way, d - 1],
            device_id={"seq": lax.rem(target + n_seq, n_seq)},
            device_id_type=MESH,
        )

    def reaches(way, d):
        return seq + d < n_seq if way == 0 else seq >= d

    def comes(way, d):
        return reaches(1 - way, d)

    def receive():
        edge_ref[:width, :] = jnp.zeros((width, width), F32)
        edge_ref[width:, :] = jnp.zeros((8, width), F32)
        for d in range(1, n_seq):
            @pl.when(comes(0, d))
            def _():
                hop(0, d).wait_recv()
                log = edge_ref[width:width + 1, :]
                scale_ref[d - 1:d, :] = log
                edge_ref[:width, :] += jnp.exp(log) * rx_ref[d - 1, :width, :]
                edge_ref[width:width + 1, :] += rx_ref[d - 1, width:width + 1, :]
        return edge_ref[:width, :]

    def receive_back():
        edge_ref[:width, :] = jnp.zeros((width, width), F32)
        for d in range(1, n_seq):
            @pl.when(comes(1, d))
            def _():
                hop(1, d).wait_recv()
                edge_ref[:width, :] += rear_rx_ref[d - 1]
        return edge_ref[:width, :]

    def send_back(far):
        for d in range(n_seq - 1, 0, -1):
            @pl.when(seq == d if far else seq > d)
            def _():
                back_ref[d - 1] = jnp.exp(scale_ref[d - 1:d, :]) * rear_ref[nblk]
                hop(1, d).start()

    def finish(way):
        for d in range(1, n_seq):
            @pl.when(reaches(way, d))
            def _():
                hop(way, d).wait_send()

    for d in range(1, n_seq):
        @pl.when(reaches(0, d))
        def _():
            hop(0, d).start()

    loads[3].wait()
    loads[5].wait()
    before = jnp.zeros((1, width), F32)
    for b in range(nblk):
        flipped_ref[b] = jnp.transpose(state_ref[b])
        scales_ref[b:b + 1, :] = jnp.exp(before)
        before = before + a_row(b)
    scales_ref[nblk:nblk + 1, :] = jnp.exp(before)
    gain_col = jnp.transpose(jnp.broadcast_to(gain_ref[...], (width, width)))
    diagonal = lax.broadcasted_iota(jnp.int32, (TILE, TILE), 0) <= lax.broadcasted_iota(
        jnp.int32, (TILE, TILE), 1
    )
    for b in range(nblk):
        vt_ref[:, span(b)] = flip(v_ref[span(b), :]).astype(BF16)
        qt = flip(q_ref[span(b), :])
        qt_ref[:, span(b)] = qt.astype(BF16)
        queried_ref[:, span(b)] = (jnp.exp(c_row(b)) * qt).astype(BF16)
        col_ref[span(b), :] = jnp.transpose(jnp.broadcast_to(c_row(b), (width, BLK)))
        for i in range(tiles):
            s0 = i * TILE
            rest = BLK - s0
            scores = dot(k_ref[span(b, s0, TILE), :], q_ref[span(b, s0, rest), :], 1, 1)
            diff = c_ref[b:b + 1, s0:] - lanes(col_ref[span(b, s0, TILE), :], rest)
            near = jnp.exp(jnp.where(diagonal, diff[:, :TILE], -jnp.inf))
            inner = near
            if rest > TILE:
                inner = jnp.concatenate([near, jnp.exp(diff[:, TILE:])], axis=1)
            inner_ref[b, s0:s0 + TILE, s0:] = inner
            mix = (inner * scores).astype(BF16)
            mix_ref[b, s0:s0 + TILE, s0:] = mix
            part = dot(vt_ref[:, span(b, s0, TILE)], mix)
            if i == 0:
                out_ref[:, span(b)] = part
            else:
                out_ref[:, span(b, s0, rest)] += part
    loads[4].wait()
    for b in range(nblk):
        scaled_ref[:, span(b)] = lanes(gain_col, BLK) * flip(y_ref[span(b), :])

    entering = receive()
    flipped = jnp.transpose(entering)
    if stat_ref.shape[0] > 2 * nblk:
        stat_ref[...] = jnp.zeros_like(stat_ref)
    for b in range(nblk):
        held = flipped_ref[b] + scales_ref[b:b + 1, :] * flipped
        carried = dot(held.astype(BF16), qt_ref[:, span(b)])
        out = out_ref[:, span(b)] + jnp.exp(c_row(b)) * carried
        out_ref[:, span(b)] = out
        stat_ref[b:b + 1, :] = jnp.sum(out * out, axis=0, keepdims=True)
        stat_ref[nblk + b:nblk + b + 1, :] = jnp.sum(
            out * scaled_ref[:, span(b)], axis=0, keepdims=True
        )

    def share(d):
        if n_head & (n_head - 1):
            partner = lax.rem(head + d, n_head)
        else:
            partner = head
            for bit in range(n_head.bit_length()):
                if d >> bit & 1:
                    partner = partner + (1 - 2 * lax.rem(head // (1 << bit), 2)) * (1 << bit)
        return pltpu.make_async_remote_copy(
            src_ref=stat_ref,
            dst_ref=stats_ref.at[d - 1],
            send_sem=hsend_sem.at[0],
            recv_sem=hrecv_sem.at[0],
            device_id={"head": partner},
            device_id_type=MESH,
        )

    shares = pltpu.make_async_remote_copy(
        src_ref=stats_ref,
        dst_ref=stats_ref,
        send_sem=hsend_sem.at[0],
        recv_sem=hrecv_sem.at[0],
        device_id={"head": lax.rem(head + 1, n_head)},
        device_id_type=MESH,
    )

    for d in sorted(range(1, n_head), key=lambda d: -(d >> 1).bit_count()):
        share(d).start()
    shares.wait_recv()
    total = stat_ref[...]
    for d in range(1, n_head):
        total = total + stats_ref[d - 1]
    inv = lax.rsqrt(total[:nblk] / features + EPS)
    coef = inv * inv * inv * total[nblk:2 * nblk] / features

    rear = jnp.zeros((width, width), F32)
    for b in range(nblk):
        dout = (
            inv[b:b + 1] * scaled_ref[:, span(b)] - out_ref[:, span(b)] * coef[b:b + 1]
        ).astype(BF16)
        dout_ref[:, span(b)] = dout
        piece = dot(queried_ref[:, span(b)], dout, 1, 1)
        rear_ref[b] = piece
        rear = rear + scales_ref[b:b + 1, :] * piece
    rear_ref[nblk] = rear
    send_back(True)

    for b in range(nblk):
        held_ref[b] = (state_ref[b] + scales_ref[b:b + 1, :] * entering).astype(BF16)
        grad_q = jnp.exp(c_row(b)) * dot(held_ref[b], dout_ref[:, span(b)])
        halves = [grad_q[:, i * TILE:(i + 1) * TILE] for i in range(tiles)]
        for i in range(tiles):
            s0 = i * TILE
            rest = BLK - s0
            dout = dout_ref[:, span(b, s0, rest)]
            dscores = dot(v_ref[span(b, s0, TILE), :], dout)
            dmix = (inner_ref[b, s0:s0 + TILE, s0:] * dscores).astype(BF16)
            part = dot(kt_ref[:, span(b, s0, TILE)], dmix)
            for j in range(i, tiles):
                halves[j] = halves[j] + part[:, (j - i) * TILE:(j - i + 1) * TILE]
            gk_ref[span(b, s0, TILE), :] = dot(dmix, q_ref[span(b, s0, rest), :])
            gv_ref[span(b, s0, TILE), :] = dot(mix_ref[b, s0:s0 + TILE, s0:], dout, 1, 1)
        for i in range(tiles):
            oq_ref[span(b, i * TILE, TILE), :] = jnp.transpose(halves[i]).astype(BF16)
        end_ref[span(b), :] = jnp.exp(a_row(b) - col_ref[span(b), :])
        if b == min(1, nblk - 1):
            send_back(False)

    rear = jnp.zeros((width, width), F32)
    for b in reversed(range(nblk)):
        piece = rear_ref[b]
        rear_ref[b] = rear
        rear = jnp.exp(a_row(b)) * rear + piece
    leaving = receive_back()
    after = jnp.zeros((1, width), F32)
    for b in reversed(range(nblk)):
        kept_ref[b] = (rear_ref[b] + jnp.exp(after) * leaving).astype(BF16)
        after = after + a_row(b)

    finish(0)
    finish(1)
    shares.wait_send()


def closing(
    oq_ref, k_ref, v_ref, gk_ref, gv_ref, end_ref, kept_ref,
    gq_hbm, gk_hbm, gv_hbm,
    ok_ref, ov_ref, out_sem,
):
    tokens = k_ref.shape[0]
    nblk = tokens // BLK

    def span(b):
        return pl.ds(b * BLK, BLK)

    first = pltpu.make_async_copy(oq_ref, gq_hbm, out_sem.at[2 * nblk])
    first.start()
    stores = []
    for b in range(nblk):
        ending = end_ref[span(b), :]
        ok_ref[span(b), :] = (
            gk_ref[span(b), :] + ending * dot(v_ref[span(b), :], kept_ref[b], 1, 1)
        ).astype(BF16)
        ov_ref[span(b), :] = (
            gv_ref[span(b), :] + ending * dot(k_ref[span(b), :], kept_ref[b])
        ).astype(BF16)
        for i, (src, dst) in enumerate(((ok_ref, gk_hbm), (ov_ref, gv_hbm))):
            store = pltpu.make_async_copy(
                src.at[span(b), :], dst.at[span(b), :], out_sem.at[2 * b + i]
            )
            store.start()
            stores.append(store)
    first.wait()
    for store in stores:
        store.wait()


def shards(n_seq, n_head, query, key, value, grad_out, log_decay, gain):
    tokens, width = query.shape
    nblk = tokens // BLK
    features = width * n_head
    rows = -(-nblk // 8) * 8
    srows = -(-2 * nblk // 8) * 8
    big = lambda dtype: pltpu.VMEM((tokens, width), dtype)
    wide = lambda dtype: pltpu.VMEM((width, tokens), dtype)
    shape = jax.ShapeDtypeStruct((tokens, width), BF16)
    hbm = pl.BlockSpec(memory_space=pl.ANY)
    vmem = pl.BlockSpec(memory_space=pltpu.VMEM)
    dma = pltpu.SemaphoreType.DMA
    kept = pltpu.VMEM((nblk, width, width), BF16)
    stay = lambda x: pltpu.with_memory_space_constraint(x, pltpu.HBM)
    middle = pl.pallas_call(
        functools.partial(kernel, n_seq, n_head, features),
        out_shape=(big(BF16), big(BF16), big(BF16), big(F32), big(F32), big(F32), kept),
        in_specs=[pl.BlockSpec(memory_space=pltpu.HBM)] * 6,
        out_specs=(vmem,) * 7,
        scratch_shapes=[
            pltpu.VMEM((1, tokens), F32), pltpu.VMEM((1, width), F32),
            big(BF16), big(BF16),
            wide(BF16), wide(BF16), wide(BF16), wide(BF16), wide(F32),
            pltpu.VMEM((rows, BLK), F32),
            pltpu.VMEM((rows, width), F32),
            big(F32),
            pltpu.VMEM((nblk, BLK, BLK), F32),
            pltpu.VMEM((nblk, BLK, BLK), BF16),
            wide(F32), wide(BF16),
            pltpu.VMEM((nblk, width, width), F32),
            pltpu.VMEM((nblk + 1, width, width), F32),
            pltpu.VMEM((nblk, width, width), BF16),
            pltpu.VMEM((width + 8, width), F32),
            pltpu.VMEM((width + 8, width), F32),
            pltpu.VMEM((n_seq - 1, width + 8, width), F32),
            pltpu.VMEM((n_seq - 1, width, width), F32),
            pltpu.VMEM((n_seq - 1, width, width), F32),
            pltpu.VMEM((n_seq, width), F32),
            pltpu.VMEM((nblk, width, width), F32),
            pltpu.VMEM((nblk + 1, width), F32),
            pltpu.VMEM((srows, BLK), F32),
            pltpu.VMEM((n_head - 1, srows, BLK), F32),
            dma((6,)),
            dma((2, n_seq - 1)), dma((2, n_seq - 1)),
            dma((1,)), dma((1,)),
        ],
        compiler_params=pltpu.CompilerParams(
            collective_id=0, has_side_effects=True, vmem_limit_bytes=40 << 20
        ),
    )(*map(stay, (query, key, value, grad_out, log_decay, gain.reshape(1, width))))
    return pl.pallas_call(
        closing,
        out_shape=(shape, shape, shape),
        in_specs=[vmem] * 7,
        out_specs=(hbm, hbm, hbm),
        scratch_shapes=[big(BF16), big(BF16), dma((2 * nblk + 1,))],
        compiler_params=pltpu.CompilerParams(vmem_limit_bytes=8 << 20),
    )(*middle)


def solution(mesh):
    return jax.shard_map(
        functools.partial(shards, mesh.shape["seq"], mesh.shape["head"]),
        mesh=mesh,
        in_specs=(
            P("seq", "head"),
            P("seq", "head"),
            P("seq", "head"),
            P("seq", "head"),
            P("head", "seq"),
            P("head"),
        ),
        out_specs=(P("seq", "head"), P("seq", "head"), P("seq", "head")),
        check_vma=False,
    )
```

```python
import functools

import jax
import jax.numpy as jnp
from jax import lax
from jax.experimental import pallas as pl
from jax.experimental.pallas import tpu as pltpu
from jax.sharding import PartitionSpec as P

BLK = 512
TILE = 256
EPS = 1e-06
F32 = jnp.float32
BF16 = jnp.bfloat16
MESH = pl.DeviceIdType.MESH


def dot(a, b, ca=1, cb=0):
    return lax.dot_general(a, b, (((ca,), (cb,)), ((), ())), preferred_element_type=F32)


def flip(x):
    n = x.shape[1]
    eye = lax.broadcasted_iota(jnp.int32, (n, n), 0) == lax.broadcasted_iota(jnp.int32, (n, n), 1)
    return dot(jnp.where(eye, 1.0, 0.0).astype(BF16), x, 1, 1)


def lanes(x, width):
    return jnp.concatenate([x] * (width // x.shape[1]), axis=1)


def kernel(
    n_seq, n_head, features,
    q_hbm, k_hbm, v_hbm, y_hbm, decay_hbm, gain_hbm,
    oq_ref, k_ref, v_ref, gk_ref, gv_ref, end_ref, kept_ref,
    decay_ref, gain_ref, q_ref, y_ref, kt_ref, qt_ref, vt_ref, queried_ref, scaled_ref,
    c_ref, a_ref, col_ref, inner_ref, mix_ref, out_ref, dout_ref,
    state_ref, rear_ref, held_ref, edge_ref,
    tx_ref, rx_ref, back_ref, rear_rx_ref, scale_ref, flipped_ref, scales_ref, stat_ref, stats_ref,
    in_sem, know_sem, send_sem, recv_sem, hsend_sem, hrecv_sem,
):
    seq = lax.axis_index("seq")
    head = lax.axis_index("head")
    tokens, width = q_ref.shape
    nblk = tokens // BLK
    tiles = BLK // TILE

    barrier = pltpu.get_barrier_semaphore()
    for step in (-1, 1):
        @pl.when((seq + step >= 0) & (seq + step < n_seq))
        def _():
            pl.semaphore_signal(
                barrier,
                inc=1,
                device_id={"seq": lax.rem(seq + step + n_seq, n_seq)},
                device_id_type=MESH,
            )
    for d in range(1, n_head):
        pl.semaphore_signal(
            barrier, inc=1, device_id={"head": lax.rem(head + d, n_head)}, device_id_type=MESH
        )

    pairs = (
        (decay_hbm, decay_ref), (k_hbm, k_ref), (v_hbm, v_ref), (q_hbm, q_ref), (y_hbm, y_ref),
        (gain_hbm, gain_ref),
    )
    loads = [
        pltpu.make_async_copy(src, dst, in_sem.at[i]) for i, (src, dst) in enumerate(pairs)
    ]
    for load in loads:
        load.start()

    def span(b, start=0, size=BLK):
        return pl.ds(b * BLK + start, size)

    rows = c_ref.shape[0]
    upper = jnp.where(
        lax.broadcasted_iota(jnp.int32, (width, width), 0)
        <= lax.broadcasted_iota(jnp.int32, (width, width), 1),
        1.0, 0.0,
    ).astype(BF16)
    pieces = BLK // width
    pad = [jnp.zeros((rows - nblk, width), F32)] if rows > nblk else []
    loads[0].wait()
    loads[1].wait()
    loads[2].wait()
    x = jnp.concatenate(
        sum(
            (
                [
                    decay_ref[:, b * BLK + j * width:b * BLK + (j + 1) * width]
                    for b in range(nblk)
                ]
                + pad
                for j in range(pieces)
            ),
            [],
        ),
        axis=0,
    )
    x1 = x.astype(BF16).astype(F32)
    x2 = (x - x1).astype(BF16).astype(F32)
    x3 = x - x1 - x2
    sums = dot(jnp.concatenate([x1, x2, x3], axis=0).astype(BF16), upper)
    size = pieces * rows
    sums = sums[:size] + sums[size:2 * size] + sums[2 * size:]
    total = jnp.zeros((rows, width), F32)
    for j in range(pieces):
        piece = sums[j * rows:(j + 1) * rows]
        c_ref[:, j * width:(j + 1) * width] = piece + total
        total = total + jnp.broadcast_to(piece[:, width - 1:], (rows, width))
    a_ref[...] = total

    def c_row(b):
        return c_ref[b:b + 1, :]

    def a_row(b):
        return a_ref[b:b + 1, :]

    keyed = []
    for b in range(nblk):
        kt = flip(k_ref[span(b), :])
        kt_ref[:, span(b)] = kt.astype(BF16)
        ending = jnp.exp(lanes(a_row(b), BLK) - c_row(b))
        keyed.append((ending * kt).astype(BF16))
    state = jnp.zeros((width, width), F32)
    own = jnp.zeros((1, width), F32)
    for b in range(nblk):
        state_ref[b] = state
        state = jnp.exp(a_row(b)) * state + dot(keyed[b], v_ref[span(b), :])
        own = own + a_row(b)
    tx_ref[:width, :] = state
    tx_ref[width:, :] = jnp.broadcast_to(own, (8, width))

    inner = (seq > 0) & (seq < n_seq - 1)

    @pl.when(inner)
    def _():
        pl.semaphore_wait(barrier, n_head + 1)

    @pl.when(jnp.logical_not(inner))
    def _():
        pl.semaphore_wait(barrier, n_head if n_seq > 1 else n_head - 1)

    def tell(d):
        pl.semaphore_signal(
            know_sem.at[d],
            inc=1,
            device_id={"seq": lax.rem(seq - 1 + n_seq, n_seq)},
            device_id_type=MESH,
        )

    if n_seq > 2:
        pl.when(inner)(lambda: tell(2))

    def hop(way, d):
        if way == 0:
            head_rows = pl.ds(0, width + 1)
            target, src, dst = seq + d, tx_ref.at[head_rows, :], rx_ref.at[d - 1, head_rows, :]
        else:
            target, src, dst = seq - d, back_ref.at[d - 1], rear_rx_ref.at[d - 1]
        return pltpu.make_async_remote_copy(
            src_ref=src,
            dst_ref=dst,
            send_sem=send_sem.at[way, d - 1],
            recv_sem=recv_sem.at[way, d - 1],
            device_id={"seq": lax.rem(target + n_seq, n_seq)},
            device_id_type=MESH,
        )

    def reaches(way, d):
        return seq + d < n_seq if way == 0 else seq >= d

    def comes(way, d):
        return reaches(1 - way, d)

    def receive():
        edge_ref[:width, :] = jnp.zeros((width, width), F32)
        edge_ref[width:, :] = jnp.zeros((8, width), F32)
        for d in range(1, n_seq):
            @pl.when(comes(0, d))
            def _():
                hop(0, d).wait_recv()
                log = edge_ref[width:width + 1, :]
                scale_ref[d - 1:d, :] = log
                edge_ref[:width, :] += jnp.exp(log) * rx_ref[d - 1, :width, :]
                edge_ref[width:width + 1, :] += rx_ref[d - 1, width:width + 1, :]
        return edge_ref[:width, :]

    def receive_back():
        edge_ref[:width, :] = jnp.zeros((width, width), F32)
        for d in range(1, n_seq):
            @pl.when(comes(1, d))
            def _():
                hop(1, d).wait_recv()
                edge_ref[:width, :] += rear_rx_ref[d - 1]
        return edge_ref[:width, :]

    def send_back(far):
        for d in range(n_seq - 1, 0, -1):
            @pl.when(seq == d if far else seq > d)
            def _():
                back_ref[d - 1] = jnp.exp(scale_ref[d - 1:d, :]) * rear_ref[nblk]
                hop(1, d).start()

    def finish(way):
        for d in range(1, n_seq):
            @pl.when(reaches(way, d))
            def _():
                hop(way, d).wait_send()

    def send(d):
        @pl.when(reaches(0, d))
        def _():
            if d > 1:
                pl.semaphore_wait(know_sem.at[d], 1)
            if d > 1 and d + 1 < n_seq:
                pl.when(seq > 0)(lambda: tell(d + 1))
            hop(0, d).start()

    if n_seq > 1:
        send(1)

    loads[3].wait()
    loads[5].wait()
    before = jnp.zeros((1, width), F32)
    for b in range(nblk):
        flipped_ref[b] = jnp.transpose(state_ref[b])
        scales_ref[b:b + 1, :] = jnp.exp(before)
        before = before + a_row(b)
    scales_ref[nblk:nblk + 1, :] = jnp.exp(before)
    gain_col = jnp.transpose(jnp.broadcast_to(gain_ref[...], (width, width)))
    diagonal = lax.broadcasted_iota(jnp.int32, (TILE, TILE), 0) <= lax.broadcasted_iota(
        jnp.int32, (TILE, TILE), 1
    )
    for b in range(nblk):
        vt_ref[:, span(b)] = flip(v_ref[span(b), :]).astype(BF16)
        qt = flip(q_ref[span(b), :])
        qt_ref[:, span(b)] = qt.astype(BF16)
        queried_ref[:, span(b)] = (jnp.exp(c_row(b)) * qt).astype(BF16)
        col_ref[span(b), :] = jnp.transpose(jnp.broadcast_to(c_row(b), (width, BLK)))
        for i in range(tiles):
            s0 = i * TILE
            rest = BLK - s0
            scores = dot(k_ref[span(b, s0, TILE), :], q_ref[span(b, s0, rest), :], 1, 1)
            diff = c_ref[b:b + 1, s0:] - lanes(col_ref[span(b, s0, TILE), :], rest)
            near = jnp.exp(jnp.where(diagonal, diff[:, :TILE], -jnp.inf))
            inner = near
            if rest > TILE:
                inner = jnp.concatenate([near, jnp.exp(diff[:, TILE:])], axis=1)
            inner_ref[b, s0:s0 + TILE, s0:] = inner
            mix = (inner * scores).astype(BF16)
            mix_ref[b, s0:s0 + TILE, s0:] = mix
            part = dot(vt_ref[:, span(b, s0, TILE)], mix)
            if i == 0:
                out_ref[:, span(b)] = part
            else:
                out_ref[:, span(b, s0, rest)] += part
        for d in range(2 + b, 3 + b if b < nblk - 1 else n_seq):
            if d < n_seq:
                send(d)
    loads[4].wait()
    for b in range(nblk):
        scaled_ref[:, span(b)] = lanes(gain_col, BLK) * flip(y_ref[span(b), :])

    entering = receive()
    flipped = jnp.transpose(entering)
    if stat_ref.shape[0] > 2 * nblk:
        stat_ref[...] = jnp.zeros_like(stat_ref)
    for b in range(nblk):
        held = flipped_ref[b] + scales_ref[b:b + 1, :] * flipped
        carried = dot(held.astype(BF16), qt_ref[:, span(b)])
        out = out_ref[:, span(b)] + jnp.exp(c_row(b)) * carried
        out_ref[:, span(b)] = out
        stat_ref[b:b + 1, :] = jnp.sum(out * out, axis=0, keepdims=True)
        stat_ref[nblk + b:nblk + b + 1, :] = jnp.sum(
            out * scaled_ref[:, span(b)], axis=0, keepdims=True
        )

    def share(d):
        if n_head & (n_head - 1):
            partner = lax.rem(head + d, n_head)
        else:
            partner = head
            for bit in range(n_head.bit_length()):
                if d >> bit & 1:
                    partner = partner + (1 - 2 * lax.rem(head // (1 << bit), 2)) * (1 << bit)
        return pltpu.make_async_remote_copy(
            src_ref=stat_ref,
            dst_ref=stats_ref.at[d - 1],
            send_sem=hsend_sem.at[0],
            recv_sem=hrecv_sem.at[0],
            device_id={"head": partner},
            device_id_type=MESH,
        )

    shares = pltpu.make_async_remote_copy(
        src_ref=stats_ref,
        dst_ref=stats_ref,
        send_sem=hsend_sem.at[0],
        recv_sem=hrecv_sem.at[0],
        device_id={"head": lax.rem(head + 1, n_head)},
        device_id_type=MESH,
    )

    for d in sorted(range(1, n_head), key=lambda d: -(d >> 1).bit_count()):
        share(d).start()
    shares.wait_recv()
    total = stat_ref[...]
    for d in range(1, n_head):
        total = total + stats_ref[d - 1]
    inv = lax.rsqrt(total[:nblk] / features + EPS)
    coef = inv * inv * inv * total[nblk:2 * nblk] / features

    rear = jnp.zeros((width, width), F32)
    for b in range(nblk):
        dout = (
            inv[b:b + 1] * scaled_ref[:, span(b)] - out_ref[:, span(b)] * coef[b:b + 1]
        ).astype(BF16)
        dout_ref[:, span(b)] = dout
        piece = dot(queried_ref[:, span(b)], dout, 1, 1)
        rear_ref[b] = piece
        rear = rear + scales_ref[b:b + 1, :] * piece
    rear_ref[nblk] = rear
    send_back(True)

    for b in range(nblk):
        held_ref[b] = (state_ref[b] + scales_ref[b:b + 1, :] * entering).astype(BF16)
        grad_q = jnp.exp(c_row(b)) * dot(held_ref[b], dout_ref[:, span(b)])
        halves = [grad_q[:, i * TILE:(i + 1) * TILE] for i in range(tiles)]
        for i in range(tiles):
            s0 = i * TILE
            rest = BLK - s0
            dout = dout_ref[:, span(b, s0, rest)]
            dscores = dot(v_ref[span(b, s0, TILE), :], dout)
            dmix = (inner_ref[b, s0:s0 + TILE, s0:] * dscores).astype(BF16)
            part = dot(kt_ref[:, span(b, s0, TILE)], dmix)
            for j in range(i, tiles):
                halves[j] = halves[j] + part[:, (j - i) * TILE:(j - i + 1) * TILE]
            gk_ref[span(b, s0, TILE), :] = dot(dmix, q_ref[span(b, s0, rest), :])
            gv_ref[span(b, s0, TILE), :] = dot(mix_ref[b, s0:s0 + TILE, s0:], dout, 1, 1)
        for i in range(tiles):
            oq_ref[span(b, i * TILE, TILE), :] = jnp.transpose(halves[i]).astype(BF16)
        end_ref[span(b), :] = jnp.exp(a_row(b) - col_ref[span(b), :])
        if b == min(1, nblk - 1):
            send_back(False)

    rear = jnp.zeros((width, width), F32)
    for b in reversed(range(nblk)):
        piece = rear_ref[b]
        rear_ref[b] = rear
        rear = jnp.exp(a_row(b)) * rear + piece
    leaving = receive_back()
    after = jnp.zeros((1, width), F32)
    for b in reversed(range(nblk)):
        kept_ref[b] = (rear_ref[b] + jnp.exp(after) * leaving).astype(BF16)
        after = after + a_row(b)

    finish(0)
    finish(1)
    shares.wait_send()


def closing(
    oq_ref, k_ref, v_ref, gk_ref, gv_ref, end_ref, kept_ref,
    gq_hbm, gk_hbm, gv_hbm,
    ok_ref, ov_ref, out_sem,
):
    tokens = k_ref.shape[0]
    nblk = tokens // BLK

    def span(b):
        return pl.ds(b * BLK, BLK)

    first = pltpu.make_async_copy(oq_ref, gq_hbm, out_sem.at[2 * nblk])
    first.start()
    stores = []
    for b in range(nblk):
        ending = end_ref[span(b), :]
        ok_ref[span(b), :] = (
            gk_ref[span(b), :] + ending * dot(v_ref[span(b), :], kept_ref[b], 1, 1)
        ).astype(BF16)
        ov_ref[span(b), :] = (
            gv_ref[span(b), :] + ending * dot(k_ref[span(b), :], kept_ref[b])
        ).astype(BF16)
        for i, (src, dst) in enumerate(((ok_ref, gk_hbm), (ov_ref, gv_hbm))):
            store = pltpu.make_async_copy(
                src.at[span(b), :], dst.at[span(b), :], out_sem.at[2 * b + i]
            )
            store.start()
            stores.append(store)
    first.wait()
    for store in stores:
        store.wait()


def shards(n_seq, n_head, query, key, value, grad_out, log_decay, gain):
    tokens, width = query.shape
    nblk = tokens // BLK
    features = width * n_head
    rows = -(-nblk // 8) * 8
    srows = -(-2 * nblk // 8) * 8
    big = lambda dtype: pltpu.VMEM((tokens, width), dtype)
    wide = lambda dtype: pltpu.VMEM((width, tokens), dtype)
    shape = jax.ShapeDtypeStruct((tokens, width), BF16)
    hbm = pl.BlockSpec(memory_space=pl.ANY)
    vmem = pl.BlockSpec(memory_space=pltpu.VMEM)
    dma = pltpu.SemaphoreType.DMA
    kept = pltpu.VMEM((nblk, width, width), BF16)
    stay = lambda x: pltpu.with_memory_space_constraint(x, pltpu.HBM)
    middle = pl.pallas_call(
        functools.partial(kernel, n_seq, n_head, features),
        out_shape=(big(BF16), big(BF16), big(BF16), big(F32), big(F32), big(F32), kept),
        in_specs=[pl.BlockSpec(memory_space=pltpu.HBM)] * 6,
        out_specs=(vmem,) * 7,
        scratch_shapes=[
            pltpu.VMEM((1, tokens), F32), pltpu.VMEM((1, width), F32),
            big(BF16), big(BF16),
            wide(BF16), wide(BF16), wide(BF16), wide(BF16), wide(F32),
            pltpu.VMEM((rows, BLK), F32),
            pltpu.VMEM((rows, width), F32),
            big(F32),
            pltpu.VMEM((nblk, BLK, BLK), F32),
            pltpu.VMEM((nblk, BLK, BLK), BF16),
            wide(F32), wide(BF16),
            pltpu.VMEM((nblk, width, width), F32),
            pltpu.VMEM((nblk + 1, width, width), F32),
            pltpu.VMEM((nblk, width, width), BF16),
            pltpu.VMEM((width + 8, width), F32),
            pltpu.VMEM((width + 8, width), F32),
            pltpu.VMEM((n_seq - 1, width + 8, width), F32),
            pltpu.VMEM((n_seq - 1, width, width), F32),
            pltpu.VMEM((n_seq - 1, width, width), F32),
            pltpu.VMEM((n_seq, width), F32),
            pltpu.VMEM((nblk, width, width), F32),
            pltpu.VMEM((nblk + 1, width), F32),
            pltpu.VMEM((srows, BLK), F32),
            pltpu.VMEM((n_head - 1, srows, BLK), F32),
            dma((6,)),
            pltpu.SemaphoreType.REGULAR((n_seq,)),
            dma((2, n_seq - 1)), dma((2, n_seq - 1)),
            dma((1,)), dma((1,)),
        ],
        compiler_params=pltpu.CompilerParams(
            collective_id=0, has_side_effects=True, vmem_limit_bytes=40 << 20
        ),
    )(*map(stay, (query, key, value, grad_out, log_decay, gain.reshape(1, width))))
    return pl.pallas_call(
        closing,
        out_shape=(shape, shape, shape),
        in_specs=[vmem] * 7,
        out_specs=(hbm, hbm, hbm),
        scratch_shapes=[big(BF16), big(BF16), dma((2 * nblk + 1,))],
        compiler_params=pltpu.CompilerParams(vmem_limit_bytes=8 << 20),
    )(*middle)


def solution(mesh):
    return jax.shard_map(
        functools.partial(shards, mesh.shape["seq"], mesh.shape["head"]),
        mesh=mesh,
        in_specs=(
            P("seq", "head"),
            P("seq", "head"),
            P("seq", "head"),
            P("seq", "head"),
            P("head", "seq"),
            P("head"),
        ),
        out_specs=(P("seq", "head"), P("seq", "head"), P("seq", "head")),
        check_vma=False,
    )
```

```python
import functools

import jax
import jax.numpy as jnp
from jax import lax
from jax.experimental import pallas as pl
from jax.experimental.pallas import tpu as pltpu
from jax.sharding import PartitionSpec as P

BLK = 512
TILE = 256
EPS = 1e-06
F32 = jnp.float32
BF16 = jnp.bfloat16
MESH = pl.DeviceIdType.MESH


def dot(a, b, ca=1, cb=0):
    return lax.dot_general(a, b, (((ca,), (cb,)), ((), ())), preferred_element_type=F32)


def flip(x):
    n = x.shape[1]
    eye = lax.broadcasted_iota(jnp.int32, (n, n), 0) == lax.broadcasted_iota(jnp.int32, (n, n), 1)
    return dot(jnp.where(eye, 1.0, 0.0).astype(BF16), x, 1, 1)


def lanes(x, width):
    return jnp.concatenate([x] * (width // x.shape[1]), axis=1)


def kernel(
    n_seq, n_head, features,
    q_hbm, k_hbm, v_hbm, y_hbm, decay_hbm, gain_hbm,
    oq_ref, k_ref, v_ref, gk_ref, gv_ref, end_ref, kept_ref,
    decay_ref, gain_ref, q_ref, y_ref, kt_ref, qt_ref, vt_ref, queried_ref, scaled_ref,
    c_ref, a_ref, col_ref, inner_ref, mix_ref, out_ref, dout_ref,
    state_ref, rear_ref, held_ref, edge_ref,
    tx_ref, rx_ref, back_ref, rear_rx_ref, scale_ref, flipped_ref, scales_ref, stat_ref, stats_ref,
    in_sem, know_sem, send_sem, recv_sem, hsend_sem, hrecv_sem,
):
    seq = lax.axis_index("seq")
    head = lax.axis_index("head")
    tokens, width = q_ref.shape
    nblk = tokens // BLK
    tiles = BLK // TILE

    barrier = pltpu.get_barrier_semaphore()
    for step in (-1, 1):
        @pl.when((seq + step >= 0) & (seq + step < n_seq))
        def _():
            pl.semaphore_signal(
                barrier,
                inc=1,
                device_id={"seq": lax.rem(seq + step + n_seq, n_seq)},
                device_id_type=MESH,
            )
    for d in range(1, n_head):
        pl.semaphore_signal(
            barrier, inc=1, device_id={"head": lax.rem(head + d, n_head)}, device_id_type=MESH
        )

    pairs = (
        (decay_hbm, decay_ref), (k_hbm, k_ref), (v_hbm, v_ref), (q_hbm, q_ref), (y_hbm, y_ref),
        (gain_hbm, gain_ref),
    )
    loads = [
        pltpu.make_async_copy(src, dst, in_sem.at[i]) for i, (src, dst) in enumerate(pairs)
    ]
    for load in loads:
        load.start()

    def span(b, start=0, size=BLK):
        return pl.ds(b * BLK + start, size)

    rows = c_ref.shape[0]
    upper = jnp.where(
        lax.broadcasted_iota(jnp.int32, (width, width), 0)
        <= lax.broadcasted_iota(jnp.int32, (width, width), 1),
        1.0, 0.0,
    ).astype(BF16)
    pieces = BLK // width
    pad = [jnp.zeros((rows - nblk, width), F32)] if rows > nblk else []
    loads[0].wait()
    loads[1].wait()
    loads[2].wait()
    x = jnp.concatenate(
        sum(
            (
                [
                    decay_ref[:, b * BLK + j * width:b * BLK + (j + 1) * width]
                    for b in range(nblk)
                ]
                + pad
                for j in range(pieces)
            ),
            [],
        ),
        axis=0,
    )
    x1 = x.astype(BF16).astype(F32)
    x2 = (x - x1).astype(BF16).astype(F32)
    x3 = x - x1 - x2
    sums = dot(jnp.concatenate([x1, x2, x3], axis=0).astype(BF16), upper)
    size = pieces * rows
    sums = sums[:size] + sums[size:2 * size] + sums[2 * size:]
    total = jnp.zeros((rows, width), F32)
    for j in range(pieces):
        piece = sums[j * rows:(j + 1) * rows]
        c_ref[:, j * width:(j + 1) * width] = piece + total
        total = total + jnp.broadcast_to(piece[:, width - 1:], (rows, width))
    a_ref[...] = total

    def c_row(b):
        return c_ref[b:b + 1, :]

    def a_row(b):
        return a_ref[b:b + 1, :]

    keyed = []
    for b in range(nblk):
        kt = flip(k_ref[span(b), :])
        kt_ref[:, span(b)] = kt.astype(BF16)
        ending = jnp.exp(lanes(a_row(b), BLK) - c_row(b))
        keyed.append((ending * kt).astype(BF16))
    state = jnp.zeros((width, width), F32)
    own = jnp.zeros((1, width), F32)
    for b in range(nblk):
        state_ref[b] = state
        state = jnp.exp(a_row(b)) * state + dot(keyed[b], v_ref[span(b), :])
        own = own + a_row(b)
    tx_ref[:width, :] = state
    tx_ref[width:, :] = jnp.broadcast_to(own, (8, width))

    inner = (seq > 0) & (seq < n_seq - 1)

    @pl.when(inner)
    def _():
        pl.semaphore_wait(barrier, n_head + 1)

    @pl.when(jnp.logical_not(inner))
    def _():
        pl.semaphore_wait(barrier, n_head if n_seq > 1 else n_head - 1)

    def tell(d):
        pl.semaphore_signal(
            know_sem.at[d],
            inc=1,
            device_id={"seq": lax.rem(seq - 1 + n_seq, n_seq)},
            device_id_type=MESH,
        )

    if n_seq > 2:
        pl.when(inner)(lambda: tell(2))

    def hop(way, d):
        if way == 0:
            head_rows = pl.ds(0, width + 1)
            target, src, dst = seq + d, tx_ref.at[head_rows, :], rx_ref.at[d - 1, head_rows, :]
        else:
            target, src, dst = seq - d, back_ref.at[d - 1], rear_rx_ref.at[d - 1]
        return pltpu.make_async_remote_copy(
            src_ref=src,
            dst_ref=dst,
            send_sem=send_sem.at[way, d - 1],
            recv_sem=recv_sem.at[way, d - 1],
            device_id={"seq": lax.rem(target + n_seq, n_seq)},
            device_id_type=MESH,
        )

    def reaches(way, d):
        return seq + d < n_seq if way == 0 else seq >= d

    def comes(way, d):
        return reaches(1 - way, d)

    def receive():
        edge_ref[:width, :] = jnp.zeros((width, width), F32)
        edge_ref[width:, :] = jnp.zeros((8, width), F32)
        for d in range(1, n_seq):
            @pl.when(comes(0, d))
            def _():
                hop(0, d).wait_recv()
                log = edge_ref[width:width + 1, :]
                scale_ref[d - 1:d, :] = log
                edge_ref[:width, :] += jnp.exp(log) * rx_ref[d - 1, :width, :]
                edge_ref[width:width + 1, :] += rx_ref[d - 1, width:width + 1, :]
        return edge_ref[:width, :]

    def receive_back():
        edge_ref[:width, :] = jnp.zeros((width, width), F32)
        for d in range(1, n_seq):
            @pl.when(comes(1, d))
            def _():
                hop(1, d).wait_recv()
                edge_ref[:width, :] += rear_rx_ref[d - 1]
        return edge_ref[:width, :]

    def send_back(far):
        for d in range(n_seq - 1, 0, -1):
            @pl.when(seq == d if far else seq > d)
            def _():
                back_ref[d - 1] = jnp.exp(scale_ref[d - 1:d, :]) * rear_ref[nblk]
                hop(1, d).start()

    def finish(way):
        for d in range(1, n_seq):
            @pl.when(reaches(way, d))
            def _():
                hop(way, d).wait_send()

    def send(d):
        @pl.when(reaches(0, d))
        def _():
            if d > 1:
                pl.semaphore_wait(know_sem.at[d], 1)
            if d > 1 and d + 1 < n_seq:
                pl.when(seq > 0)(lambda: tell(d + 1))
            hop(0, d).start()

    if n_seq > 1:
        send(1)

    loads[3].wait()
    loads[5].wait()
    before = jnp.zeros((1, width), F32)
    for b in range(nblk):
        flipped_ref[b] = jnp.transpose(state_ref[b])
        scales_ref[b:b + 1, :] = jnp.exp(before)
        before = before + a_row(b)
    scales_ref[nblk:nblk + 1, :] = jnp.exp(before)
    gain_col = jnp.transpose(jnp.broadcast_to(gain_ref[...], (width, width)))
    diagonal = lax.broadcasted_iota(jnp.int32, (TILE, TILE), 0) <= lax.broadcasted_iota(
        jnp.int32, (TILE, TILE), 1
    )
    for b in range(nblk):
        vt_ref[:, span(b)] = flip(v_ref[span(b), :]).astype(BF16)
        qt = flip(q_ref[span(b), :])
        qt_ref[:, span(b)] = qt.astype(BF16)
        queried_ref[:, span(b)] = (jnp.exp(c_row(b)) * qt).astype(BF16)
        col_ref[span(b), :] = jnp.transpose(jnp.broadcast_to(c_row(b), (width, BLK)))
        for i in range(tiles):
            s0 = i * TILE
            rest = BLK - s0
            scores = dot(k_ref[span(b, s0, TILE), :], q_ref[span(b, s0, rest), :], 1, 1)
            diff = c_ref[b:b + 1, s0:] - lanes(col_ref[span(b, s0, TILE), :], rest)
            near = jnp.exp(jnp.where(diagonal, diff[:, :TILE], -jnp.inf))
            inner = near
            if rest > TILE:
                inner = jnp.concatenate([near, jnp.exp(diff[:, TILE:])], axis=1)
            inner_ref[b, s0:s0 + TILE, s0:] = inner
            mix = (inner * scores).astype(BF16)
            mix_ref[b, s0:s0 + TILE, s0:] = mix
            part = dot(vt_ref[:, span(b, s0, TILE)], mix)
            if i == 0:
                out_ref[:, span(b)] = part
            else:
                out_ref[:, span(b, s0, rest)] += part
        for d in range(2 + b, 3 + b if b < nblk - 1 else n_seq):
            if d < n_seq:
                send(d)
    loads[4].wait()
    for b in range(nblk):
        scaled_ref[:, span(b)] = lanes(gain_col, BLK) * flip(y_ref[span(b), :])

    entering = receive()
    flipped = jnp.transpose(entering)
    if stat_ref.shape[0] > 2 * nblk:
        stat_ref[...] = jnp.zeros_like(stat_ref)
    for b in range(nblk):
        held = flipped_ref[b] + scales_ref[b:b + 1, :] * flipped
        carried = dot(held.astype(BF16), qt_ref[:, span(b)])
        out = out_ref[:, span(b)] + jnp.exp(c_row(b)) * carried
        out_ref[:, span(b)] = out
        stat_ref[b:b + 1, :] = jnp.sum(out * out, axis=0, keepdims=True)
        stat_ref[nblk + b:nblk + b + 1, :] = jnp.sum(
            out * scaled_ref[:, span(b)], axis=0, keepdims=True
        )

    def share(d):
        if n_head & (n_head - 1):
            partner = lax.rem(head + d, n_head)
        else:
            partner = head
            for bit in range(n_head.bit_length()):
                if d >> bit & 1:
                    partner = partner + (1 - 2 * lax.rem(head // (1 << bit), 2)) * (1 << bit)
        return pltpu.make_async_remote_copy(
            src_ref=stat_ref,
            dst_ref=stats_ref.at[d - 1],
            send_sem=hsend_sem.at[0],
            recv_sem=hrecv_sem.at[0],
            device_id={"head": partner},
            device_id_type=MESH,
        )

    shares = pltpu.make_async_remote_copy(
        src_ref=stats_ref,
        dst_ref=stats_ref,
        send_sem=hsend_sem.at[0],
        recv_sem=hrecv_sem.at[0],
        device_id={"head": lax.rem(head + 1, n_head)},
        device_id_type=MESH,
    )

    for d in sorted(range(1, n_head), key=lambda d: -(d >> 1).bit_count()):
        share(d).start()
    shares.wait_recv()
    total = stat_ref[...]
    for d in range(1, n_head):
        total = total + stats_ref[d - 1]
    inv = lax.rsqrt(total[:nblk] / features + EPS)
    coef = inv * inv * inv * total[nblk:2 * nblk] / features

    rear = jnp.zeros((width, width), F32)
    for b in range(nblk):
        dout = (
            inv[b:b + 1] * scaled_ref[:, span(b)] - out_ref[:, span(b)] * coef[b:b + 1]
        ).astype(BF16)
        dout_ref[:, span(b)] = dout
        piece = dot(queried_ref[:, span(b)], dout, 1, 1)
        rear_ref[b] = piece
        rear = rear + scales_ref[b:b + 1, :] * piece
    rear_ref[nblk] = rear
    send_back(True)
    pl.when(seq < n_seq - 1)(lambda: send_back(False))

    for b in range(nblk):
        held_ref[b] = (state_ref[b] + scales_ref[b:b + 1, :] * entering).astype(BF16)
        grad_q = jnp.exp(c_row(b)) * dot(held_ref[b], dout_ref[:, span(b)])
        halves = [grad_q[:, i * TILE:(i + 1) * TILE] for i in range(tiles)]
        for i in range(tiles):
            s0 = i * TILE
            rest = BLK - s0
            dout = dout_ref[:, span(b, s0, rest)]
            dscores = dot(v_ref[span(b, s0, TILE), :], dout)
            dmix = (inner_ref[b, s0:s0 + TILE, s0:] * dscores).astype(BF16)
            part = dot(kt_ref[:, span(b, s0, TILE)], dmix)
            for j in range(i, tiles):
                halves[j] = halves[j] + part[:, (j - i) * TILE:(j - i + 1) * TILE]
            gk_ref[span(b, s0, TILE), :] = dot(dmix, q_ref[span(b, s0, rest), :])
            gv_ref[span(b, s0, TILE), :] = dot(mix_ref[b, s0:s0 + TILE, s0:], dout, 1, 1)
        for i in range(tiles):
            oq_ref[span(b, i * TILE, TILE), :] = jnp.transpose(halves[i]).astype(BF16)
        end_ref[span(b), :] = jnp.exp(a_row(b) - col_ref[span(b), :])
        if b == min(2, nblk - 1):
            pl.when(seq == n_seq - 1)(lambda: send_back(False))

    rear = jnp.zeros((width, width), F32)
    for b in reversed(range(nblk)):
        piece = rear_ref[b]
        rear_ref[b] = rear
        rear = jnp.exp(a_row(b)) * rear + piece
    leaving = receive_back()
    after = jnp.zeros((1, width), F32)
    for b in reversed(range(nblk)):
        kept_ref[b] = (rear_ref[b] + jnp.exp(after) * leaving).astype(BF16)
        after = after + a_row(b)

    finish(0)
    finish(1)
    shares.wait_send()


def closing(
    oq_ref, k_ref, v_ref, gk_ref, gv_ref, end_ref, kept_ref,
    gq_hbm, gk_hbm, gv_hbm,
    ok_ref, ov_ref, out_sem,
):
    tokens = k_ref.shape[0]
    nblk = tokens // BLK

    def span(b):
        return pl.ds(b * BLK, BLK)

    first = pltpu.make_async_copy(oq_ref, gq_hbm, out_sem.at[2 * nblk])
    first.start()
    stores = []
    for b in range(nblk):
        ending = end_ref[span(b), :]
        ok_ref[span(b), :] = (
            gk_ref[span(b), :] + ending * dot(v_ref[span(b), :], kept_ref[b], 1, 1)
        ).astype(BF16)
        ov_ref[span(b), :] = (
            gv_ref[span(b), :] + ending * dot(k_ref[span(b), :], kept_ref[b])
        ).astype(BF16)
        for i, (src, dst) in enumerate(((ok_ref, gk_hbm), (ov_ref, gv_hbm))):
            store = pltpu.make_async_copy(
                src.at[span(b), :], dst.at[span(b), :], out_sem.at[2 * b + i]
            )
            store.start()
            stores.append(store)
    first.wait()
    for store in stores:
        store.wait()


def shards(n_seq, n_head, query, key, value, grad_out, log_decay, gain):
    tokens, width = query.shape
    nblk = tokens // BLK
    features = width * n_head
    rows = -(-nblk // 8) * 8
    srows = -(-2 * nblk // 8) * 8
    big = lambda dtype: pltpu.VMEM((tokens, width), dtype)
    wide = lambda dtype: pltpu.VMEM((width, tokens), dtype)
    shape = jax.ShapeDtypeStruct((tokens, width), BF16)
    hbm = pl.BlockSpec(memory_space=pl.ANY)
    vmem = pl.BlockSpec(memory_space=pltpu.VMEM)
    dma = pltpu.SemaphoreType.DMA
    kept = pltpu.VMEM((nblk, width, width), BF16)
    stay = lambda x: pltpu.with_memory_space_constraint(x, pltpu.HBM)
    middle = pl.pallas_call(
        functools.partial(kernel, n_seq, n_head, features),
        out_shape=(big(BF16), big(BF16), big(BF16), big(F32), big(F32), big(F32), kept),
        in_specs=[pl.BlockSpec(memory_space=pltpu.HBM)] * 6,
        out_specs=(vmem,) * 7,
        scratch_shapes=[
            pltpu.VMEM((1, tokens), F32), pltpu.VMEM((1, width), F32),
            big(BF16), big(BF16),
            wide(BF16), wide(BF16), wide(BF16), wide(BF16), wide(F32),
            pltpu.VMEM((rows, BLK), F32),
            pltpu.VMEM((rows, width), F32),
            big(F32),
            pltpu.VMEM((nblk, BLK, BLK), F32),
            pltpu.VMEM((nblk, BLK, BLK), BF16),
            wide(F32), wide(BF16),
            pltpu.VMEM((nblk, width, width), F32),
            pltpu.VMEM((nblk + 1, width, width), F32),
            pltpu.VMEM((nblk, width, width), BF16),
            pltpu.VMEM((width + 8, width), F32),
            pltpu.VMEM((width + 8, width), F32),
            pltpu.VMEM((n_seq - 1, width + 8, width), F32),
            pltpu.VMEM((n_seq - 1, width, width), F32),
            pltpu.VMEM((n_seq - 1, width, width), F32),
            pltpu.VMEM((n_seq, width), F32),
            pltpu.VMEM((nblk, width, width), F32),
            pltpu.VMEM((nblk + 1, width), F32),
            pltpu.VMEM((srows, BLK), F32),
            pltpu.VMEM((n_head - 1, srows, BLK), F32),
            dma((6,)),
            pltpu.SemaphoreType.REGULAR((n_seq,)),
            dma((2, n_seq - 1)), dma((2, n_seq - 1)),
            dma((1,)), dma((1,)),
        ],
        compiler_params=pltpu.CompilerParams(
            collective_id=0, has_side_effects=True, vmem_limit_bytes=40 << 20
        ),
    )(*map(stay, (query, key, value, grad_out, log_decay, gain.reshape(1, width))))
    return pl.pallas_call(
        closing,
        out_shape=(shape, shape, shape),
        in_specs=[vmem] * 7,
        out_specs=(hbm, hbm, hbm),
        scratch_shapes=[big(BF16), big(BF16), dma((2 * nblk + 1,))],
        compiler_params=pltpu.CompilerParams(vmem_limit_bytes=8 << 20),
    )(*middle)


def solution(mesh):
    return jax.shard_map(
        functools.partial(shards, mesh.shape["seq"], mesh.shape["head"]),
        mesh=mesh,
        in_specs=(
            P("seq", "head"),
            P("seq", "head"),
            P("seq", "head"),
            P("seq", "head"),
            P("head", "seq"),
            P("head"),
        ),
        out_specs=(P("seq", "head"), P("seq", "head"), P("seq", "head")),
        check_vma=False,
    )
```

```python
import functools

import jax
import jax.numpy as jnp
from jax import lax
from jax.experimental import pallas as pl
from jax.experimental.pallas import tpu as pltpu
from jax.sharding import PartitionSpec as P

BLK = 512
TILE = 256
EPS = 1e-06
F32 = jnp.float32
BF16 = jnp.bfloat16
MESH = pl.DeviceIdType.MESH


def dot(a, b, ca=1, cb=0):
    return lax.dot_general(a, b, (((ca,), (cb,)), ((), ())), preferred_element_type=F32)


def flip(x):
    n = x.shape[1]
    eye = lax.broadcasted_iota(jnp.int32, (n, n), 0) == lax.broadcasted_iota(jnp.int32, (n, n), 1)
    return dot(jnp.where(eye, 1.0, 0.0).astype(BF16), x, 1, 1)


def lanes(x, width):
    return jnp.concatenate([x] * (width // x.shape[1]), axis=1)


def kernel(
    n_seq, n_head, features,
    q_hbm, k_hbm, v_hbm, y_hbm, decay_hbm, gain_hbm,
    oq_ref, k_ref, v_ref, gk_ref, gv_ref, end_ref, kept_ref,
    decay_ref, gain_ref, q_ref, y_ref, kt_ref, qt_ref, vt_ref, queried_ref, scaled_ref,
    c_ref, a_ref, col_ref, inner_ref, mix_ref, out_ref, dout_ref,
    state_ref, rear_ref, held_ref, edge_ref,
    tx_ref, rx_ref, back_ref, rear_rx_ref, scale_ref, flipped_ref, scales_ref, stat_ref, stats_ref,
    in_sem, know_sem, send_sem, recv_sem, hsend_sem, hrecv_sem,
):
    seq = lax.axis_index("seq")
    head = lax.axis_index("head")
    tokens, width = q_ref.shape
    nblk = tokens // BLK
    tiles = BLK // TILE

    barrier = pltpu.get_barrier_semaphore()
    for step in (-1, 1):
        @pl.when((seq + step >= 0) & (seq + step < n_seq))
        def _():
            pl.semaphore_signal(
                barrier,
                inc=1,
                device_id={"seq": lax.rem(seq + step + n_seq, n_seq)},
                device_id_type=MESH,
            )
    for d in range(1, n_head):
        pl.semaphore_signal(
            barrier, inc=1, device_id={"head": lax.rem(head + d, n_head)}, device_id_type=MESH
        )

    pairs = (
        (decay_hbm, decay_ref), (k_hbm, k_ref), (v_hbm, v_ref), (q_hbm, q_ref), (y_hbm, y_ref),
        (gain_hbm, gain_ref),
    )
    loads = [
        pltpu.make_async_copy(src, dst, in_sem.at[i]) for i, (src, dst) in enumerate(pairs)
    ]
    for load in loads:
        load.start()

    def span(b, start=0, size=BLK):
        return pl.ds(b * BLK + start, size)

    rows = c_ref.shape[0]
    upper = jnp.where(
        lax.broadcasted_iota(jnp.int32, (width, width), 0)
        <= lax.broadcasted_iota(jnp.int32, (width, width), 1),
        1.0, 0.0,
    ).astype(BF16)
    pieces = BLK // width
    pad = [jnp.zeros((rows - nblk, width), F32)] if rows > nblk else []
    loads[0].wait()
    loads[1].wait()
    loads[2].wait()
    x = jnp.concatenate(
        sum(
            (
                [
                    decay_ref[:, b * BLK + j * width:b * BLK + (j + 1) * width]
                    for b in range(nblk)
                ]
                + pad
                for j in range(pieces)
            ),
            [],
        ),
        axis=0,
    )
    x1 = x.astype(BF16).astype(F32)
    x2 = (x - x1).astype(BF16).astype(F32)
    x3 = x - x1 - x2
    sums = dot(jnp.concatenate([x1, x2, x3], axis=0).astype(BF16), upper)
    size = pieces * rows
    sums = sums[:size] + sums[size:2 * size] + sums[2 * size:]
    total = jnp.zeros((rows, width), F32)
    for j in range(pieces):
        piece = sums[j * rows:(j + 1) * rows]
        c_ref[:, j * width:(j + 1) * width] = piece + total
        total = total + jnp.broadcast_to(piece[:, width - 1:], (rows, width))
    a_ref[...] = total

    def c_row(b):
        return c_ref[b:b + 1, :]

    def a_row(b):
        return a_ref[b:b + 1, :]

    keyed = []
    for b in range(nblk):
        kt = flip(k_ref[span(b), :])
        kt_ref[:, span(b)] = kt.astype(BF16)
        ending = jnp.exp(lanes(a_row(b), BLK) - c_row(b))
        keyed.append((ending * kt).astype(BF16))
    state = jnp.zeros((width, width), F32)
    own = jnp.zeros((1, width), F32)
    for b in range(nblk):
        state_ref[b] = state
        state = jnp.exp(a_row(b)) * state + dot(keyed[b], v_ref[span(b), :])
        own = own + a_row(b)
    tx_ref[:width, :] = state
    tx_ref[width:, :] = jnp.broadcast_to(own, (8, width))

    inner = (seq > 0) & (seq < n_seq - 1)

    @pl.when(inner)
    def _():
        pl.semaphore_wait(barrier, n_head + 1)

    @pl.when(jnp.logical_not(inner))
    def _():
        pl.semaphore_wait(barrier, n_head if n_seq > 1 else n_head - 1)

    def tell(d):
        pl.semaphore_signal(
            know_sem.at[d],
            inc=1,
            device_id={"seq": lax.rem(seq - 1 + n_seq, n_seq)},
            device_id_type=MESH,
        )

    if n_seq > 2:
        pl.when(inner)(lambda: tell(2))

    def hop(way, d):
        if way == 0:
            head_rows = pl.ds(0, width + 1)
            target, src, dst = seq + d, tx_ref.at[head_rows, :], rx_ref.at[d - 1, head_rows, :]
        else:
            target, src, dst = seq - d, back_ref.at[d - 1], rear_rx_ref.at[d - 1]
        return pltpu.make_async_remote_copy(
            src_ref=src,
            dst_ref=dst,
            send_sem=send_sem.at[way, d - 1],
            recv_sem=recv_sem.at[way, d - 1],
            device_id={"seq": lax.rem(target + n_seq, n_seq)},
            device_id_type=MESH,
        )

    def reaches(way, d):
        return seq + d < n_seq if way == 0 else seq >= d

    def comes(way, d):
        return reaches(1 - way, d)

    def receive():
        edge_ref[:width, :] = jnp.zeros((width, width), F32)
        edge_ref[width:, :] = jnp.zeros((8, width), F32)
        for d in range(1, n_seq):
            @pl.when(comes(0, d))
            def _():
                hop(0, d).wait_recv()
                log = edge_ref[width:width + 1, :]
                scale_ref[d - 1:d, :] = log
                edge_ref[:width, :] += jnp.exp(log) * rx_ref[d - 1, :width, :]
                edge_ref[width:width + 1, :] += rx_ref[d - 1, width:width + 1, :]
        return edge_ref[:width, :]

    def receive_back():
        edge_ref[:width, :] = jnp.zeros((width, width), F32)
        for d in range(1, n_seq):
            @pl.when(comes(1, d))
            def _():
                hop(1, d).wait_recv()
                edge_ref[:width, :] += rear_rx_ref[d - 1]
        return edge_ref[:width, :]

    def send_back(far):
        for d in range(n_seq - 1, 0, -1):
            @pl.when(seq == d if far else seq > d)
            def _():
                back_ref[d - 1] = jnp.exp(scale_ref[d - 1:d, :]) * rear_ref[nblk]
                hop(1, d).start()

    def finish(way):
        for d in range(1, n_seq):
            @pl.when(reaches(way, d))
            def _():
                hop(way, d).wait_send()

    def send(d):
        @pl.when(reaches(0, d))
        def _():
            if d > 1:
                pl.semaphore_wait(know_sem.at[d], 1)
            if d > 1 and d + 1 < n_seq:
                pl.when(seq > 0)(lambda: tell(d + 1))
            hop(0, d).start()

    if n_seq > 1:
        send(1)

    loads[3].wait()
    loads[5].wait()
    before = jnp.zeros((1, width), F32)
    for b in range(nblk):
        flipped_ref[b] = jnp.transpose(state_ref[b])
        scales_ref[b:b + 1, :] = jnp.exp(before)
        before = before + a_row(b)
    scales_ref[nblk:nblk + 1, :] = jnp.exp(before)
    gain_col = jnp.transpose(jnp.broadcast_to(gain_ref[...], (width, width)))
    diagonal = lax.broadcasted_iota(jnp.int32, (TILE, TILE), 0) <= lax.broadcasted_iota(
        jnp.int32, (TILE, TILE), 1
    )
    for b in range(nblk):
        vt_ref[:, span(b)] = flip(v_ref[span(b), :]).astype(BF16)
        qt = flip(q_ref[span(b), :])
        qt_ref[:, span(b)] = qt.astype(BF16)
        queried_ref[:, span(b)] = (jnp.exp(c_row(b)) * qt).astype(BF16)
        col_ref[span(b), :] = jnp.transpose(jnp.broadcast_to(c_row(b), (width, BLK)))
        for i in range(tiles):
            s0 = i * TILE
            rest = BLK - s0
            scores = dot(k_ref[span(b, s0, TILE), :], q_ref[span(b, s0, rest), :], 1, 1)
            diff = c_ref[b:b + 1, s0:] - lanes(col_ref[span(b, s0, TILE), :], rest)
            near = jnp.exp(jnp.where(diagonal, diff[:, :TILE], -jnp.inf))
            inner = near
            if rest > TILE:
                inner = jnp.concatenate([near, jnp.exp(diff[:, TILE:])], axis=1)
            inner_ref[b, s0:s0 + TILE, s0:] = inner
            mix = (inner * scores).astype(BF16)
            mix_ref[b, s0:s0 + TILE, s0:] = mix
            part = dot(vt_ref[:, span(b, s0, TILE)], mix)
            if i == 0:
                out_ref[:, span(b)] = part
            else:
                out_ref[:, span(b, s0, rest)] += part
        for d in range(2 + b, 3 + b if b < nblk - 1 else n_seq):
            if d < n_seq:
                send(d)
    loads[4].wait()
    for b in range(nblk):
        scaled_ref[:, span(b)] = lanes(gain_col, BLK) * flip(y_ref[span(b), :])

    entering = receive()
    flipped = jnp.transpose(entering)
    if stat_ref.shape[0] > 2 * nblk:
        stat_ref[...] = jnp.zeros_like(stat_ref)
    for b in range(nblk):
        held = flipped_ref[b] + scales_ref[b:b + 1, :] * flipped
        carried = dot(held.astype(BF16), qt_ref[:, span(b)])
        out = out_ref[:, span(b)] + jnp.exp(c_row(b)) * carried
        out_ref[:, span(b)] = out
        stat_ref[b:b + 1, :] = jnp.sum(out * out, axis=0, keepdims=True)
        stat_ref[nblk + b:nblk + b + 1, :] = jnp.sum(
            out * scaled_ref[:, span(b)], axis=0, keepdims=True
        )

    def share(d):
        if n_head & (n_head - 1):
            partner = lax.rem(head + d, n_head)
        else:
            partner = head
            for bit in range(n_head.bit_length()):
                if d >> bit & 1:
                    partner = partner + (1 - 2 * lax.rem(head // (1 << bit), 2)) * (1 << bit)
        return pltpu.make_async_remote_copy(
            src_ref=stat_ref,
            dst_ref=stats_ref.at[d - 1],
            send_sem=hsend_sem.at[0],
            recv_sem=hrecv_sem.at[0],
            device_id={"head": partner},
            device_id_type=MESH,
        )

    shares = pltpu.make_async_remote_copy(
        src_ref=stats_ref,
        dst_ref=stats_ref,
        send_sem=hsend_sem.at[0],
        recv_sem=hrecv_sem.at[0],
        device_id={"head": lax.rem(head + 1, n_head)},
        device_id_type=MESH,
    )

    for d in sorted(range(1, n_head), key=lambda d: -(d >> 1).bit_count()):
        share(d).start()
    shares.wait_recv()
    total = stat_ref[...]
    for d in range(1, n_head):
        total = total + stats_ref[d - 1]
    inv = lax.rsqrt(total[:nblk] / features + EPS)
    coef = inv * inv * inv * total[nblk:2 * nblk] / features

    rear = jnp.zeros((width, width), F32)
    for b in range(nblk):
        dout = (
            inv[b:b + 1] * scaled_ref[:, span(b)] - out_ref[:, span(b)] * coef[b:b + 1]
        ).astype(BF16)
        dout_ref[:, span(b)] = dout
        piece = dot(queried_ref[:, span(b)], dout, 1, 1)
        rear_ref[b] = piece
        rear = rear + scales_ref[b:b + 1, :] * piece
    rear_ref[nblk] = rear
    send_back(True)
    pl.when(seq < n_seq - 1)(lambda: send_back(False))

    for b in range(nblk):
        held_ref[b] = (state_ref[b] + scales_ref[b:b + 1, :] * entering).astype(BF16)
        grad_q = jnp.exp(c_row(b)) * dot(held_ref[b], dout_ref[:, span(b)])
        halves = [grad_q[:, i * TILE:(i + 1) * TILE] for i in range(tiles)]
        for i in range(tiles):
            s0 = i * TILE
            rest = BLK - s0
            dout = dout_ref[:, span(b, s0, rest)]
            dscores = dot(v_ref[span(b, s0, TILE), :], dout)
            dmix = (inner_ref[b, s0:s0 + TILE, s0:] * dscores).astype(BF16)
            part = dot(kt_ref[:, span(b, s0, TILE)], dmix)
            for j in range(i, tiles):
                halves[j] = halves[j] + part[:, (j - i) * TILE:(j - i + 1) * TILE]
            gk_ref[span(b, s0, TILE), :] = dot(dmix, q_ref[span(b, s0, rest), :])
            gv_ref[span(b, s0, TILE), :] = dot(mix_ref[b, s0:s0 + TILE, s0:], dout, 1, 1)
        for i in range(tiles):
            oq_ref[span(b, i * TILE, TILE), :] = jnp.transpose(halves[i]).astype(BF16)
        end_ref[span(b), :] = jnp.exp(a_row(b) - col_ref[span(b), :])
        if b == min(2, nblk - 1):
            pl.when(seq == n_seq - 1)(lambda: send_back(False))

    rear = jnp.zeros((width, width), F32)
    for b in reversed(range(nblk)):
        piece = rear_ref[b]
        rear_ref[b] = rear
        rear = jnp.exp(a_row(b)) * rear + piece
    leaving = receive_back()
    after = jnp.zeros((1, width), F32)
    for b in reversed(range(nblk)):
        kept_ref[b] = (rear_ref[b] + jnp.exp(after) * leaving).astype(BF16)
        after = after + a_row(b)

    finish(0)
    finish(1)
    shares.wait_send()


def closing(
    oq_ref, k_ref, v_ref, gk_ref, gv_ref, end_ref, kept_ref,
    gq_hbm, gk_hbm, gv_hbm,
    ok_ref, ov_ref, out_sem,
):
    tokens = k_ref.shape[0]
    nblk = tokens // BLK

    def span(b):
        return pl.ds(b * BLK, BLK)

    first = pltpu.make_async_copy(oq_ref, gq_hbm, out_sem.at[2 * nblk])
    first.start()
    stores = []
    for b in range(nblk):
        ending = end_ref[span(b), :]
        by_value = dot(v_ref[span(b), :], kept_ref[b], 1, 1)
        by_key = dot(k_ref[span(b), :], kept_ref[b])
        ok_ref[span(b), :] = (gk_ref[span(b), :] + ending * by_value).astype(BF16)
        ov_ref[span(b), :] = (gv_ref[span(b), :] + ending * by_key).astype(BF16)
        for i, (src, dst) in enumerate(((ok_ref, gk_hbm), (ov_ref, gv_hbm))):
            store = pltpu.make_async_copy(
                src.at[span(b), :], dst.at[span(b), :], out_sem.at[2 * b + i]
            )
            store.start()
            stores.append(store)
    first.wait()
    for store in stores:
        store.wait()


def shards(n_seq, n_head, query, key, value, grad_out, log_decay, gain):
    tokens, width = query.shape
    nblk = tokens // BLK
    features = width * n_head
    rows = -(-nblk // 8) * 8
    srows = -(-2 * nblk // 8) * 8
    big = lambda dtype: pltpu.VMEM((tokens, width), dtype)
    wide = lambda dtype: pltpu.VMEM((width, tokens), dtype)
    shape = jax.ShapeDtypeStruct((tokens, width), BF16)
    hbm = pl.BlockSpec(memory_space=pl.ANY)
    vmem = pl.BlockSpec(memory_space=pltpu.VMEM)
    dma = pltpu.SemaphoreType.DMA
    kept = pltpu.VMEM((nblk, width, width), BF16)
    stay = lambda x: pltpu.with_memory_space_constraint(x, pltpu.HBM)
    middle = pl.pallas_call(
        functools.partial(kernel, n_seq, n_head, features),
        out_shape=(big(BF16), big(BF16), big(BF16), big(F32), big(F32), big(F32), kept),
        in_specs=[pl.BlockSpec(memory_space=pltpu.HBM)] * 6,
        out_specs=(vmem,) * 7,
        scratch_shapes=[
            pltpu.VMEM((1, tokens), F32), pltpu.VMEM((1, width), F32),
            big(BF16), big(BF16),
            wide(BF16), wide(BF16), wide(BF16), wide(BF16), wide(F32),
            pltpu.VMEM((rows, BLK), F32),
            pltpu.VMEM((rows, width), F32),
            big(F32),
            pltpu.VMEM((nblk, BLK, BLK), F32),
            pltpu.VMEM((nblk, BLK, BLK), BF16),
            wide(F32), wide(BF16),
            pltpu.VMEM((nblk, width, width), F32),
            pltpu.VMEM((nblk + 1, width, width), F32),
            pltpu.VMEM((nblk, width, width), BF16),
            pltpu.VMEM((width + 8, width), F32),
            pltpu.VMEM((width + 8, width), F32),
            pltpu.VMEM((n_seq - 1, width + 8, width), F32),
            pltpu.VMEM((n_seq - 1, width, width), F32),
            pltpu.VMEM((n_seq - 1, width, width), F32),
            pltpu.VMEM((n_seq, width), F32),
            pltpu.VMEM((nblk, width, width), F32),
            pltpu.VMEM((nblk + 1, width), F32),
            pltpu.VMEM((srows, BLK), F32),
            pltpu.VMEM((n_head - 1, srows, BLK), F32),
            dma((6,)),
            pltpu.SemaphoreType.REGULAR((n_seq,)),
            dma((2, n_seq - 1)), dma((2, n_seq - 1)),
            dma((1,)), dma((1,)),
        ],
        compiler_params=pltpu.CompilerParams(
            collective_id=0, has_side_effects=True, vmem_limit_bytes=40 << 20
        ),
    )(*map(stay, (query, key, value, grad_out, log_decay, gain.reshape(1, width))))
    return pl.pallas_call(
        closing,
        out_shape=(shape, shape, shape),
        in_specs=[vmem] * 7,
        out_specs=(hbm, hbm, hbm),
        scratch_shapes=[big(BF16), big(BF16), dma((2 * nblk + 1,))],
        compiler_params=pltpu.CompilerParams(vmem_limit_bytes=8 << 20),
    )(*middle)


def solution(mesh):
    return jax.shard_map(
        functools.partial(shards, mesh.shape["seq"], mesh.shape["head"]),
        mesh=mesh,
        in_specs=(
            P("seq", "head"),
            P("seq", "head"),
            P("seq", "head"),
            P("seq", "head"),
            P("head", "seq"),
            P("head"),
        ),
        out_specs=(P("seq", "head"), P("seq", "head"), P("seq", "head")),
        check_vma=False,
    )
```
